32 devices in a mesh: lat: 4 (over z), lon: 8 (over y, x, core).
Axes of the slice: x: 2, y: 2, z: 4, core: 2. Of those that a mesh axis runs over, the one named last changes fastest.
Arguments:
- increments: bfloat16 [65536, 3, 128], P(('lat', 'lon')), may hold values from -6 to 6
- cotangent: bfloat16 [65536, 128], P(('lat', 'lon')), may hold values from -6 to 6
- owner_perm: int32 [32, 2048], P(('lat', 'lon')), may hold values from 0 to 2047, each once within a row
- coarse_index: int32 [2, 32768], P(None, ('lat', 'lon')), may hold values from 0 to 2047
- coarse_weight: float32 [32768], P(('lat', 'lon')), may hold values from 0.2 to 0.8
- back_index: int32 [2, 65536], P(None, ('lat', 'lon')), may hold values from 0 to 1023
- back_weight: float32 [65536], P(('lat', 'lon')), may hold values from 0.2 to 0.8
- lw_scale: float32 [16, 32768], P(None, ('lat', 'lon')), may hold values from 0.1 to 1
- sw_scale: float32 [14, 32768], P(None, ('lat', 'lon')), may hold values from 0.2 to 2
- sunlit: int32 [32768], P(('lat', 'lon')), may hold values from 0 to 1, as said below
- lw_table: bfloat16 [16, 3, 128, 128], P(None, None, 'lon'), may hold values from -0.3125 to 0.3125
- sw_table: bfloat16 [14, 3, 128, 128], P(None, None, 'lon'), may hold values from -0.3125 to 0.3125
Outputs:
- tendency: bfloat16 [65536, 128], P(('lat', 'lon'))
- gradient: bfloat16 [65536, 3, 128], P(('lat', 'lon'))
The draws below stay inside these ranges and needn't reach their ends.
Inputs may be any that keep to these rules, and one draw needn't show every extreme that they name: In each device's block of 1024 radiation columns at most 640 are sunlit, and some device has exactly 640.
All inputs are finite; a program needn't handle non-finite values.
Results may differ from the reference program's by a relative error of at most 0.014.
Values may be sent and summed in bfloat16 or wider, within the bound.
A program may use at most 64 MiB of HBM per device.

```python
import math
import jax
import jax.numpy as jnp
from jax import lax

COLS_DEV = 2048
LEV = 128
VARS = 3
BANDS_LW = 16
BANDS_SW = 14
RC_DEV = 1024
SUNMAX = 640
COLS = 65536
RCOLS = 32768
N_LAT = 4
N_LON = 8
DEVICES = 32


def draw_sunlit(key, part):
    key_count, key_full, key_order = jax.random.split(key, 3)
    counts = jax.random.randint(key_count, (DEVICES,), SUNMAX // 8, SUNMAX + 1)
    chosen = jax.random.randint(key_full, (), 0, DEVICES)
    counts = jnp.where(jnp.arange(DEVICES) == chosen, SUNMAX, counts)
    scores = jax.random.randint(key_order, (DEVICES, RC_DEV), 0, 1 << 18) * RC_DEV + jnp.arange(RC_DEV, dtype=jnp.int32)[None, :]
    ranks = jnp.argsort(jnp.argsort(scores, axis=1), axis=1)
    return (ranks < counts[:, None]).astype(jnp.int32).reshape(-1)


def place_ends(values, own_key, smallest, top_value):
    dims = values.shape
    spot = [jax.random.randint(jax.random.fold_in(own_key, axis), (), 0, dims[axis]) for axis in range(len(dims))]
    values = values.at[tuple(spot)].set(smallest)
    longest = dims.index(max(dims))
    spot[longest] = (spot[longest] + 1) % dims[longest]
    return values.at[tuple(spot)].set(top_value)


def block_levels(own_key, shape, cuts, low, high):
    factor_of, own = 1.0, jax.random.fold_in(own_key, 6)
    for axis_at, shards_of in cuts:
        heights = jnp.exp(jax.random.uniform(jax.random.fold_in(own, axis_at), (shards_of,), jnp.float32, low / len(cuts), high / len(cuts)))
        factor_of = factor_of * jnp.repeat(heights, shape[axis_at] // shards_of).reshape([-1 if axis == axis_at else 1 for axis in range(len(shape))])
    return factor_of


def scatter_about(stream_key, shape, deviation, bound, cuts=(), kind=jnp.bfloat16):
    array = jax.random.normal(stream_key, shape, jnp.float32) * deviation
    if len(cuts) > 0:
        array = block_levels(stream_key, shape, cuts, -0.22, 0.18) * array
    return jnp.clip(array, min=-bound, max=bound).astype(kind)


def setup_inputs(seed: int = 0) -> dict:
    splits = jax.random.split(jax.random.key(seed), 13)
    increments = scatter_about(splits[0], (COLS, VARS, LEV), 1.0, 6.0, ((0, 32),))
    cotangent = scatter_about(splits[1], (COLS, LEV), 1.0, 6.0, ((0, 32),))
    owner_perm = jax.vmap(lambda own: jax.random.permutation(own, COLS_DEV))(jax.random.split(splits[2], DEVICES)).reshape((DEVICES, COLS_DEV)).astype(jnp.int32)
    coarse_index = place_ends(jax.random.randint(splits[3], (2, RCOLS), 0, COLS_DEV), jax.random.fold_in(splits[3], 1), 0, COLS_DEV - 1).astype(jnp.int32)
    coarse_weight = jnp.clip(0.2 + 0.6 * jax.random.uniform(splits[4], (RCOLS,), jnp.float32) ** block_levels(splits[4], (RCOLS,), ((0, 32),), -0.2, 0.2), 0.2, 0.8)
    back_index = place_ends(jax.random.randint(splits[5], (2, COLS), 0, RC_DEV), jax.random.fold_in(splits[5], 1), 0, RC_DEV - 1).astype(jnp.int32)
    back_weight = jnp.clip(0.2 + 0.6 * jax.random.uniform(splits[6], (COLS,), jnp.float32) ** block_levels(splits[6], (COLS,), ((0, 32),), -0.2, 0.2), 0.2, 0.8)
    lw_scale = jnp.clip(jnp.exp(math.log(1.0) - 2.3025851 * jax.random.uniform(splits[7], (BANDS_LW, RCOLS), jnp.float32) ** block_levels(splits[7], (BANDS_LW, RCOLS), ((1, 32),), -0.2, 0.2)), 0.1, 1.0)
    sw_scale = jnp.clip(jnp.exp(math.log(2.0) - 2.3025851 * jax.random.uniform(splits[8], (BANDS_SW, RCOLS), jnp.float32) ** block_levels(splits[8], (BANDS_SW, RCOLS), ((1, 32),), -0.2, 0.2)), 0.2, 2.0)
    sunlit = draw_sunlit(jax.random.fold_in(splits[12], 71), 0)
    lw_table = scatter_about(splits[10], (BANDS_LW, VARS, LEV, LEV), (VARS * LEV) ** -0.5, 0.3125, ((2, 8),))
    sw_table = scatter_about(splits[11], (BANDS_SW, VARS, LEV, LEV), (VARS * LEV) ** -0.5, 0.3125, ((2, 8),))
    return {"increments": increments, "cotangent": cotangent, "owner_perm": owner_perm, "coarse_index": coarse_index, "coarse_weight": coarse_weight, "back_index": back_index, "back_weight": back_weight, "lw_scale": lw_scale, "sw_scale": sw_scale, "sunlit": sunlit, "lw_table": lw_table, "sw_table": sw_table}


def band_sum(coarse, band_table, band_scale):
    product = jnp.einsum("rc,bck->rbk", coarse.astype(jnp.float32), band_table.astype(jnp.float32))
    return jnp.einsum("br,rbk->rk", band_scale, product)


def band_adjoint(adjoint_coarse, band_table, band_scale):
    lifted = (band_scale.T[:, :, None] * adjoint_coarse[:, None, :]).astype(jnp.bfloat16)
    lifted = lax.optimization_barrier(lifted)
    return jnp.einsum("rbk,bck->rc", lifted.astype(jnp.float32), band_table.astype(jnp.float32))


def radiate(fields, cot_rad, coarse_index, coarse_weight, back_index, back_weight, lw_scale, sw_scale, sunlit, lw_bands, sw_bands):
    row_count = coarse_weight.shape[0]
    col_count = back_weight.shape[0]
    flat_rows = fields.reshape(col_count, -1)
    first = flat_rows[coarse_index[0]].astype(jnp.float32)
    second = flat_rows[coarse_index[1]].astype(jnp.float32)
    coarse = (coarse_weight[:, None] * first + (1.0 - coarse_weight)[:, None] * second).astype(jnp.bfloat16)
    sw_weight = sw_scale * sunlit.astype(jnp.float32)[None, :]
    heating = band_sum(coarse, lw_bands, lw_scale) + band_sum(coarse, sw_bands, sw_weight)
    tendency_rad = (back_weight[:, None] * heating[back_index[0]] + (1.0 - back_weight)[:, None] * heating[back_index[1]]).astype(jnp.bfloat16)
    cot_float = cot_rad.astype(jnp.float32)
    adjoint_coarse = jax.ops.segment_sum(
        jnp.concatenate([back_weight[:, None] * cot_float, (1.0 - back_weight)[:, None] * cot_float]),
        jnp.concatenate([back_index[0], back_index[1]]), num_segments=row_count)
    adjoint_rows = band_adjoint(adjoint_coarse, lw_bands, lw_scale) + band_adjoint(adjoint_coarse, sw_bands, sw_weight)
    gradient_rad = jax.ops.segment_sum(
        jnp.concatenate([coarse_weight[:, None] * adjoint_rows, (1.0 - coarse_weight)[:, None] * adjoint_rows]),
        jnp.concatenate([coarse_index[0], coarse_index[1]]), num_segments=col_count).astype(jnp.bfloat16)
    return tendency_rad, gradient_rad.reshape(fields.shape)


def pick_rows(values, order_map):
    return values[order_map]


def restore_rows(values, order_map):
    return jnp.zeros_like(values).at[order_map].set(values)


def reference(increments, cotangent, owner_perm, coarse_index, coarse_weight, back_index, back_weight, lw_scale, sw_scale, sunlit, lw_table, sw_table):
    device_count = N_LAT * N_LON
    segment = COLS_DEV // device_count

    def relay(values):
        rest = values.shape[2:]
        return values.reshape((device_count, device_count, segment) + rest).swapaxes(0, 1).reshape((device_count, COLS_DEV) + rest)

    fields_model = increments.reshape(device_count, COLS_DEV, VARS, LEV)
    cot_model = cotangent.reshape(device_count, COLS_DEV, LEV)
    fields = relay(jax.vmap(pick_rows)(fields_model, owner_perm))
    cot_rad = relay(jax.vmap(pick_rows)(cot_model, owner_perm))
    coarse_dev = coarse_index.reshape(2, device_count, RC_DEV).swapaxes(0, 1)
    coarse_wdev = coarse_weight.reshape(device_count, RC_DEV)
    back_dev = back_index.reshape(2, device_count, COLS_DEV).swapaxes(0, 1)
    back_wdev = back_weight.reshape(device_count, COLS_DEV)
    lw_dev = lw_scale.reshape(BANDS_LW, device_count, RC_DEV).swapaxes(0, 1)
    sw_dev = sw_scale.reshape(BANDS_SW, device_count, RC_DEV).swapaxes(0, 1)
    sun_dev = sunlit.reshape(device_count, RC_DEV)
    lw_bands = lw_table.reshape(BANDS_LW, VARS * LEV, LEV)
    sw_bands = sw_table.reshape(BANDS_SW, VARS * LEV, LEV)

    def one_device(item):
        return radiate(item[0], item[1], item[2], item[3], item[4], item[5], item[6], item[7], item[8], lw_bands, sw_bands)

    tendency_rad, gradient_rad = lax.map(one_device, (fields, cot_rad, coarse_dev, coarse_wdev, back_dev, back_wdev, lw_dev, sw_dev, sun_dev))
    tendency = jax.vmap(restore_rows)(relay(tendency_rad), owner_perm)
    gradient = jax.vmap(restore_rows)(relay(gradient_rad), owner_perm)
    return tendency.reshape(COLS, LEV), gradient.reshape(COLS, VARS, LEV)
```

```python
import jax
import jax.numpy as jnp
from jax import lax
from jax.experimental import pallas as pl
from jax.experimental.pallas import tpu as pltpu
from jax.sharding import PartitionSpec as P

BLOCK = 256


def lane_iota(rows, width):
    return lax.broadcasted_iota(jnp.int32, (rows, width), 1)


def row_iota(rows, width, start):
    return lax.broadcasted_iota(jnp.int32, (rows, width), 0) + start


def pick(hit):
    return jnp.where(hit, 1.0, 0.0).astype(jnp.bfloat16)


def blend(hit_first, hit_second, share):
    first = jnp.where(hit_first, share, 0.0)
    second = jnp.where(hit_second, 1.0 - share, 0.0)
    return (first + second).astype(jnp.bfloat16)


def dot(left, right):
    return lax.dot_general(left, right, (((1,), (0,)), ((), ())), preferred_element_type=jnp.float32)


def column_of(values):
    return jnp.transpose(jnp.broadcast_to(values, (8, values.shape[1])))[:, 0:1]


def radiate_kernel(
    perm_ref,
    inc_ref,
    cot_ref,
    back_ref,
    back_w,
    lw_scale,
    sw_scale,
    sun_ref,
    lw_ref,
    sw_ref,
    coarse_ref,
    coarse_w,
    tend_done,
    grad_done,
    back,
    stacked,
    cot_out,
    cot_in,
    fields_out,
    fields_in,
    grad_out,
    grad_in,
    tend_out,
    tend_in,
    tabs,
    wide,
    adj,
    heat,
    up_out,
    up_in,
    down_out,
    down_in,
    own,
    scale_in,
    coarse_in,
    share_in,
    back_in,
    back_share,
    send_sem,
    recv_sem,
    chain_send,
    chain_recv,
    meta_send,
    meta_recv,
    tab_send,
    tab_recv,
):
    var_count, col_count, width = inc_ref.shape
    planes, lon_count, segment = cot_out.shape[0], cot_out.shape[1], cot_out.shape[2]
    part = lon_count * segment
    row_count = lw_scale.shape[1]
    lw_count = lw_ref.shape[0]
    band_count = lw_count + sw_ref.shape[0]
    flat_width = var_count * width
    per_block = BLOCK // segment
    part_blocks = part // BLOCK
    row_blocks = row_count // BLOCK
    lat, lon = lax.axis_index("lat"), lax.axis_index("lon")
    parity = lax.rem(lon, 2)
    partner = lon + 1 - 2 * parity
    home = lax.div(lon, per_block)
    groups = (pl.ds(0, lw_count), pl.ds(lw_count, band_count - lw_count))

    def remote(source, landing, send, recv, target_lat, target_lon):
        return pltpu.make_async_remote_copy(
            src_ref=source,
            dst_ref=landing,
            send_sem=send,
            recv_sem=recv,
            device_id=(target_lat, target_lon),
            device_id_type=pl.DeviceIdType.MESH,
        )

    def table_copy(group, slot, target, hop):
        piece = tabs.at[slot, groups[group]]
        return remote(piece, piece, tab_send.at[group, hop, target], tab_recv.at[group, slot], lat, target)

    def copy(kind, source, landing, block, target, slot):
        return remote(source, landing, send_sem.at[kind, block, target], recv_sem.at[kind, block, slot], lat, target)

    def start_block(kind, source, landing, block, step):
        for k in range(per_block):
            target = step * per_block + k

            @pl.when(target != lon)
            def _():
                copy(kind, source.at[block, target], landing.at[block, lon], block, target, lon).start()

            @pl.when(target == lon)
            def _():
                landing[block, lon] = source[block, lon]

    def wait_block(kind, landing, block):
        @pl.loop(1, lon_count)
        def _(k):
            source = lax.rem(lon + k, lon_count)
            piece = landing.at[block, source]
            copy(kind, piece, piece, block, source, source).wait_recv()

    def wait_sent(kind, source):
        @pl.loop(0, planes)
        def _(block):
            @pl.loop(1, lon_count)
            def _(k):
                target = lax.rem(lon + k, lon_count)
                piece = source.at[block, target]
                copy(kind, piece, piece, block, target, target).wait_send()

    def meta_copy(kind, target, slot):
        span = pl.ds(pl.multiple_of(target * part, part), part)
        source, landing = (
            (back_ref.at[:, span], back_in.at[slot]),
            (back_w.at[:, span], back_share.at[slot]),
            (coarse_ref, coarse_in.at[slot]),
            (coarse_w, share_in.at[slot]),
            (scale_in.at[slot], scale_in.at[slot]),
        )[kind]
        return remote(source, landing, meta_send.at[kind, target], meta_recv.at[kind, slot], target, lon)

    def wait_meta(kinds):
        @pl.loop(1, planes)
        def _(k):
            source = lax.rem(lat + k, planes)
            for kind in kinds:
                meta_copy(kind, source, source).wait_recv()

    def chain_copy(kind, upward, block):
        out, landing, way = (up_out, up_in, 0) if upward else (down_out, down_in, 1)
        target = lat + 1 if upward else lat - 1
        piece, spot = out.at[kind, block], landing.at[kind, block]
        return remote(piece, spot, chain_send.at[kind, way, block], chain_recv.at[kind, way, block], target, lon)

    def chain_begin(kind, block):
        if planes == 1:
            return

        @pl.when(lat == 0)
        def _():
            up_out[kind, block] = own[kind, block].astype(jnp.bfloat16)
            chain_copy(kind, True, block).start()

        @pl.when(lat == planes - 1)
        def _():
            down_out[kind, block] = own[kind, block].astype(jnp.bfloat16)
            chain_copy(kind, False, block).start()

    def chain_hop(kind, hop, block):
        @pl.when(lat == hop)
        def _():
            chain_copy(kind, True, block).wait_recv()
            up_out[kind, block] = (own[kind, block] + up_in[kind, block].astype(jnp.float32)).astype(jnp.bfloat16)
            chain_copy(kind, True, block).start()

        @pl.when(lat == planes - 1 - hop)
        def _():
            chain_copy(kind, False, block).wait_recv()
            down_out[kind, block] = (own[kind, block] + down_in[kind, block].astype(jnp.float32)).astype(jnp.bfloat16)
            chain_copy(kind, False, block).start()

    def chain_after(kind, block):
        for hop in range(1, planes - 1):

            @pl.when(block >= hop - 1)
            def _():
                chain_hop(kind, hop, block - hop + 1)

    def chain_rest(kind):
        for late in range(planes, 2 * planes - 2):
            for hop in range(1, planes - 1):
                if 0 <= late - hop + 1 < planes:
                    chain_hop(kind, hop, late - hop + 1)

    def chain_ready(kind, block):
        if planes == 1:
            return

        @pl.when(lat == 0)
        def _():
            chain_copy(kind, False, block).wait_recv()

        @pl.when(lat == planes - 1)
        def _():
            chain_copy(kind, True, block).wait_recv()

    def chain_total(kind, block, rows):
        ends = up_in[kind, block, rows, :].astype(jnp.float32) + down_in[kind, block, rows, :].astype(jnp.float32)
        return own[kind, block, rows, :] + ends

    def chain_sent(kind):
        @pl.loop(0, planes)
        def _(block):
            @pl.when(lat < planes - 1)
            def _():
                chain_copy(kind, True, block).wait_send()

            @pl.when(lat > 0)
            def _():
                chain_copy(kind, False, block).wait_send()

    def scale_of(block, rows):
        turned = jnp.transpose(scale_in[block, :, rows])
        return [turned[:, b : b + 1] for b in range(band_count)]

    def sub_rows(step):
        return pl.ds(pl.multiple_of(step * BLOCK, BLOCK), BLOCK)

    tabs[lon, groups[0]] = lw_ref[...]
    tabs[lon, groups[1]] = sw_ref[...]
    for j in range(1, lon_count // 2):
        target = lax.rem(lon + 2 * j, lon_count)
        table_copy(0, lon, target, 0).start()
    table_copy(0, lon, partner, 0).start()

    scale_in[lat, pl.ds(0, lw_count)] = lw_scale[...]
    scale_in[lat, pl.ds(lw_count, band_count - lw_count)] = sw_scale[...] * sun_ref[...].astype(jnp.float32)
    scale_in[lat, pl.ds(band_count, scale_in.shape[1] - band_count)] = jnp.zeros(
        (scale_in.shape[1] - band_count, row_count), jnp.float32
    )
    span = pl.ds(pl.multiple_of(lat * part, part), part)
    back_in[lat] = back_ref[:, span]
    back_share[lat] = back_w[:, span]
    coarse_in[lat] = coarse_ref[...]
    share_in[lat] = coarse_w[...]

    @pl.loop(1, planes)
    def _(k):
        for kind in range(5):
            meta_copy(kind, lax.rem(lat + k, planes), lat).start()

    @pl.when(lat == 0)
    def _():
        up_in[...] = jnp.zeros_like(up_in)

    @pl.when(lat == planes - 1)
    def _():
        down_in[...] = jnp.zeros_like(down_in)

    stacked[:, pl.ds(0, width)] = cot_ref[...]
    for v in range(var_count):
        stacked[:, pl.ds((v + 1) * width, width)] = inc_ref[v]

    @pl.loop(0, planes)
    def _(block):
        @pl.loop(0, part_blocks)
        def _(turn):
            step = lax.rem(turn + home + 1, part_blocks)
            rows = sub_rows(block * part_blocks + step)
            table = pick(column_of(perm_ref[:, rows]) == lane_iota(BLOCK, col_count))
            moved = dot(table, stacked[...]).astype(jnp.bfloat16)
            spot = pl.ds(step * per_block, per_block)
            cot_out[block, spot] = moved[:, :width].reshape(per_block, segment, width)
            fields_out[block, spot] = moved[:, width:].reshape(per_block, segment, flat_width)
            start_block(0, cot_out, cot_in, block, step)

    for j in range(1, lon_count // 2):
        target = lax.rem(lon + 2 * j, lon_count)
        table_copy(1, lon, target, 0).start()
    table_copy(1, lon, partner, 0).start()

    @pl.loop(0, planes)
    def _(block):
        @pl.loop(0, part_blocks)
        def _(turn):
            start_block(1, fields_out, fields_in, block, lax.rem(turn + home + 1, part_blocks))

    wait_meta((0, 1))

    @pl.loop(0, planes)
    def _(block):
        wait_block(0, cot_in, block)

        @pl.loop(0, row_blocks)
        def _(step):
            rows = sub_rows(step)
            spot = row_iota(BLOCK, part, step * BLOCK)
            index = back_in[block]
            table = blend(index[0:1, :] == spot, index[1:2, :] == spot, back_share[block])
            own[0, block, rows, :] = dot(table, cot_in[block].reshape(part, width))

        chain_begin(0, block)

    for group in range(2):
        for j in range(1, lon_count // 2):
            source = lax.rem(lon + 2 * j, lon_count)
            table_copy(group, source, source, 0).wait_recv()
            table_copy(group, source, partner, 1 + j).start()

    @pl.loop(0, col_count // BLOCK)
    def _(step):
        back[sub_rows(step), :] = pick(perm_ref[...] == row_iota(BLOCK, col_count, step * BLOCK))

    for group in range(2):
        for j in range(lon_count // 2):
            source = lax.rem(partner + 2 * j, lon_count)
            table_copy(group, source, source, 0).wait_recv()
    depth = lw_ref.shape[2]
    for b in range(band_count):
        for v in range(var_count):
            piece = tabs[:, b, v].reshape(lon_count * depth, width)
            wide[pl.ds(v * lon_count * depth, lon_count * depth), pl.ds(b * width, width)] = piece
    wait_meta((2, 3, 4))

    @pl.loop(0, planes)
    def _(block):
        wait_block(1, fields_in, block)

        @pl.loop(0, row_blocks)
        def _(step):
            rows = sub_rows(step)
            spot = lane_iota(BLOCK, part) + lat * part
            first, second = column_of(coarse_in[block, 0:1, rows]), column_of(coarse_in[block, 1:2, rows])
            table = blend(first == spot, second == spot, column_of(share_in[block, :, rows]))
            coarse = dot(table, fields_in[block].reshape(part, flat_width)).astype(jnp.bfloat16)
            scale = scale_of(block, rows)
            total = jnp.zeros((BLOCK, width), jnp.float32)
            for b in range(0, band_count, 2):
                pair = dot(coarse, wide[:, b * width : (b + 2) * width])
                total = total + scale[b] * pair[:, :width] + scale[b + 1] * pair[:, width:]
            own[1, block, rows, :] = total

        chain_begin(1, block)
        chain_after(0, block)

    chain_rest(0)

    @pl.loop(0, planes)
    def _(block):
        chain_ready(0, block)

        @pl.loop(0, row_blocks)
        def _(step):
            rows = sub_rows(step)
            coarse = chain_total(0, block, rows)
            scale = scale_of(block, rows)
            lifted = jnp.concatenate([(scale[b] * coarse).astype(jnp.bfloat16) for b in range(band_count)], axis=1)
            out = lax.dot_general(lifted, wide[...], (((1,), (1,)), ((), ())), preferred_element_type=jnp.float32)
            adj[rows, :] = out.astype(jnp.bfloat16)

        @pl.loop(0, part_blocks)
        def _(turn):
            step = lax.rem(turn + home + 1, part_blocks)
            spot = row_iota(BLOCK, row_count, lat * part + step * BLOCK)
            index = coarse_in[block]
            table = blend(index[0:1, :] == spot, index[1:2, :] == spot, share_in[block])
            moved = dot(table, adj[...]).astype(jnp.bfloat16)
            grad_out[block, pl.ds(step * per_block, per_block)] = moved.reshape(per_block, segment, flat_width)
            start_block(2, grad_out, grad_in, block, step)

        chain_after(1, block)

    chain_rest(1)

    @pl.loop(0, planes)
    def _(block):
        chain_ready(1, block)
        heat[...] = chain_total(1, block, pl.ds(0, row_count)).astype(jnp.bfloat16)

        @pl.loop(0, part_blocks)
        def _(turn):
            step = lax.rem(turn + home + 1, part_blocks)
            rows = sub_rows(step)
            spot = lane_iota(BLOCK, row_count)
            first, second = column_of(back_in[block, 0:1, rows]), column_of(back_in[block, 1:2, rows])
            table = blend(first == spot, second == spot, column_of(back_share[block, :, rows]))
            moved = dot(table, heat[...]).astype(jnp.bfloat16)
            tend_out[block, pl.ds(step * per_block, per_block)] = moved.reshape(per_block, segment, width)
            start_block(3, tend_out, tend_in, block, step)

    @pl.loop(0, planes)
    def _(block):
        wait_block(2, grad_in, block)

    @pl.loop(0, col_count // BLOCK)
    def _(step):
        rows = sub_rows(step)
        moved = dot(back[rows, :], grad_in[...].reshape(col_count, flat_width)).astype(jnp.bfloat16)
        for v in range(var_count):
            grad_done[v, rows, :] = moved[:, v * width : (v + 1) * width]

    @pl.loop(0, planes)
    def _(block):
        wait_block(3, tend_in, block)

    @pl.loop(0, col_count // BLOCK)
    def _(step):
        rows = sub_rows(step)
        tend_done[rows, :] = dot(back[rows, :], tend_in[...].reshape(col_count, width)).astype(jnp.bfloat16)

    for group in range(2):
        for j in range(1, lon_count // 2):
            other = lax.rem(lon + 2 * j, lon_count)
            table_copy(group, lon, other, 0).wait_send()
            table_copy(group, other, partner, 1 + j).wait_send()
        table_copy(group, lon, partner, 0).wait_send()

    @pl.loop(1, planes)
    def _(k):
        for kind in range(5):
            meta_copy(kind, lax.rem(lat + k, planes), lat).wait_send()

    chain_sent(0)
    chain_sent(1)
    wait_sent(0, cot_out)
    wait_sent(1, fields_out)
    wait_sent(2, grad_out)
    wait_sent(3, tend_out)


def run(kernel, outs, scratch, flops, args, sems):
    shapes = [jax.ShapeDtypeStruct(shape, jnp.bfloat16) for shape in outs]
    vmem = pl.BlockSpec(memory_space=pltpu.VMEM)
    return pl.pallas_call(
        kernel,
        out_shape=shapes,
        in_specs=[vmem] * len(args),
        out_specs=[vmem] * len(outs),
        scratch_shapes=[pltpu.VMEM(shape, kind) for shape, kind in scratch] + [pltpu.SemaphoreType.DMA(shape) for shape in sems],
        compiler_params=pltpu.CompilerParams(vmem_limit_bytes=56 * 1024 * 1024, has_side_effects=True),
        cost_estimate=pl.CostEstimate(flops=flops, bytes_accessed=4 << 20, transcendentals=0),
    )(*args)


def local(
    increments,
    cotangent,
    owner_perm,
    coarse_index,
    coarse_weight,
    back_index,
    back_weight,
    lw_scale,
    sw_scale,
    sunlit,
    lw_table,
    sw_table,
    *,
    planes,
    lon_count,
):
    col_count, var_count, width = increments.shape
    row_count = coarse_weight.shape[0]
    segment = col_count // (planes * lon_count)
    part = lon_count * segment
    flat_width = var_count * width
    thin, thick = (planes, lon_count, segment, width), (planes, lon_count, segment, flat_width)
    bands = lw_table.shape[0] + sw_table.shape[0]
    scale_rows = -(-(bands + 1) // 8) * 8
    wire = (2, planes, row_count, width)
    half, full, whole = jnp.bfloat16, jnp.float32, jnp.int32
    tendency, gradient = run(
        radiate_kernel,
        [(col_count, width), (var_count, col_count, width)],
        [
            ((col_count, col_count), half),
            ((col_count, (var_count + 1) * width), half),
            (thin, half),
            (thin, half),
            (thick, half),
            (thick, half),
            (thick, half),
            (thick, half),
            (thin, half),
            (thin, half),
            ((lon_count, bands) + lw_table.shape[1:], half),
            ((flat_width, bands * width), half),
            ((row_count, flat_width), half),
            ((row_count, width), half),
            (wire, half),
            (wire, half),
            (wire, half),
            (wire, half),
            (wire, full),
            ((planes, scale_rows, row_count), full),
            ((planes, 2, row_count), whole),
            ((planes, 1, row_count), full),
            ((planes, 2, part), whole),
            ((planes, 1, part), full),
        ],
        6 * planes * row_count * bands * flat_width * width,
        (
            owner_perm,
            jnp.transpose(increments, (1, 0, 2)),
            cotangent,
            back_index,
            back_weight[None, :],
            lw_scale,
            sw_scale,
            sunlit[None, :],
            lw_table,
            sw_table,
            coarse_index,
            coarse_weight[None, :],
        ),
        (
            (4, planes, lon_count),
            (4, planes, lon_count),
            (2, 2, planes),
            (2, 2, planes),
            (5, planes),
            (5, planes),
            (2, lon_count // 2 + 1, lon_count),
            (2, lon_count),
        ),
    )
    return (tendency, jnp.transpose(gradient, (1, 0, 2)))


def solution(mesh):
    in_specs = (
        P(("lat", "lon"), None, None),
        P(("lat", "lon"), None),
        P(("lat", "lon"), None),
        P(None, ("lat", "lon")),
        P(("lat", "lon")),
        P(None, ("lat", "lon")),
        P(("lat", "lon")),
        P(None, ("lat", "lon")),
        P(None, ("lat", "lon")),
        P(("lat", "lon")),
        P(None, None, "lon", None),
        P(None, None, "lon", None),
    )
    out_specs = (P(("lat", "lon"), None), P(("lat", "lon"), None, None))

    def body(*args):
        return local(*args, planes=mesh.shape["lat"], lon_count=mesh.shape["lon"])

    return jax.shard_map(body, mesh=mesh, in_specs=in_specs, out_specs=out_specs, check_vma=False)
```

```python
import jax
import jax.numpy as jnp
from jax import lax
from jax.experimental import pallas as pl
from jax.experimental.pallas import tpu as pltpu
from jax.sharding import PartitionSpec as P

BLOCK = 256
FINAL = 512
BUNCH = 3
WIDE_SUMS = 4096


def lane_iota(rows, width):
    return lax.broadcasted_iota(jnp.int32, (rows, width), 1)


def row_iota(rows, width, start):
    return lax.broadcasted_iota(jnp.int32, (rows, width), 0) + start


def pick(hit):
    return jnp.where(hit, 1.0, 0.0).astype(jnp.bfloat16)


def blend(hit_first, hit_second, share):
    first = jnp.where(hit_first, share, 0.0)
    second = jnp.where(hit_second, 1.0 - share, 0.0)
    return (first + second).astype(jnp.bfloat16)


def dot(left, right):
    return lax.dot_general(left, right, (((1,), (0,)), ((), ())), preferred_element_type=jnp.float32)


def column_of(values):
    return jnp.transpose(jnp.broadcast_to(values, (8, values.shape[1])))[:, 0:1]


def radiate_kernel(
    perm_ref,
    inc_ref,
    cot_ref,
    back_ref,
    back_w,
    lw_scale,
    sw_scale,
    sun_ref,
    lw_ref,
    sw_ref,
    coarse_ref,
    coarse_w,
    result_in,
    stacked,
    cot_out,
    cot_in,
    fields_out,
    fields_in,
    grad_out,
    tend_out,
    tabs,
    wide,
    turned,
    ctab,
    btab,
    fields_t,
    adj,
    heat,
    up_out,
    up_in,
    down_out,
    down_in,
    own,
    scale_in,
    coarse_in,
    share_in,
    back_in,
    back_share,
    send_sem,
    recv_sem,
    chain_send,
    chain_recv,
    meta_send,
    meta_recv,
    tab_send,
    tab_recv,
):
    var_count, col_count, width = inc_ref.shape
    planes, lon_count, segment = cot_out.shape[0], cot_out.shape[1], cot_out.shape[2]
    part = lon_count * segment
    row_count = lw_scale.shape[1]
    lw_count = lw_ref.shape[0]
    band_count = lw_count + sw_ref.shape[0]
    flat_width = var_count * width
    row_blocks = row_count // BLOCK
    units = planes * row_blocks
    lat, lon = lax.axis_index("lat"), lax.axis_index("lon")
    parity = lax.rem(lon, 2)
    partner = lon + 1 - 2 * parity
    groups = (pl.ds(0, lw_count), pl.ds(lw_count, band_count - lw_count))

    def remote(source, landing, send, recv, target_lat, target_lon):
        return pltpu.make_async_remote_copy(
            src_ref=source,
            dst_ref=landing,
            send_sem=send,
            recv_sem=recv,
            device_id=(target_lat, target_lon),
            device_id_type=pl.DeviceIdType.MESH,
        )

    def table_copy(group, slot, target, hop):
        piece = tabs.at[slot, groups[group]]
        return remote(piece, piece, tab_send.at[group, hop, target], tab_recv.at[group, slot], lat, target)

    quad = lon_count == 8
    if quad:
        across = lon + 2 - 4 * lax.rem(lax.div(lon, 2), 2)
        along = lon + 4 - 8 * lax.div(lon, 4)
        near, far = (across, along), across + along - lon
    else:
        near, far = tuple(lax.rem(lon + 2 * j, lon_count) for j in range(1, lon_count // 2)), None

    def relay(group, done):
        @pl.when(parity == 0)
        def _():
            piece = table_copy(group, near[0], near[1], 1)
            piece.wait_send() if done else piece.start()

        @pl.when(parity == 1)
        def _():
            piece = table_copy(group, near[1], near[0], 1)
            piece.wait_send() if done else piece.start()

    def table_start(group):
        for target in near + (partner,):
            table_copy(group, lon, target, 0).start()

    def table_relay(group):
        for source in near:
            table_copy(group, source, source, 0).wait_recv()
        if quad:
            relay(group, False)
        for j, source in enumerate(near):
            table_copy(group, source, partner, 2 + j).start()

    def table_finish(group):
        if quad:
            table_copy(group, far, far, 0).wait_recv()
            table_copy(group, far, partner, 2 + len(near)).start()

    def table_wait(group):
        for j in range(lon_count // 2):
            source = lax.rem(partner + 2 * j, lon_count)
            table_copy(group, source, source, 0).wait_recv()

    def table_sent(group):
        for target in near + (partner,):
            table_copy(group, lon, target, 0).wait_send()
        if quad:
            relay(group, True)
        for j, source in enumerate(near + ((far,) if quad else ())):
            table_copy(group, source, partner, 2 + j).wait_send()

    def copy(kind, source, landing, block, target, slot):
        return remote(source, landing, send_sem.at[kind, block, target], recv_sem.at[kind, block, slot], lat, target)

    def start_block(kind, source, landing, block):
        landing.at[block, lon][...] = source[block, lon]

        @pl.loop(1, lon_count)
        def _(k):
            target = lax.rem(lon + k, lon_count)
            copy(kind, source.at[block, target], landing.at[block, lon], block, target, lon).start()

    def wait_block(kind, landing, block):
        @pl.loop(1, lon_count)
        def _(k):
            source = lax.rem(lon + k, lon_count)
            piece = landing.at[block, source]
            copy(kind, piece, piece, block, source, source).wait_recv()

    def wait_sent(kind, source):
        @pl.loop(0, planes)
        def _(block):
            @pl.loop(1, lon_count)
            def _(k):
                target = lax.rem(lon + k, lon_count)
                piece = source.at[block, target]
                copy(kind, piece, piece, block, target, target).wait_send()

    def meta_copy(kind, target, slot):
        span = pl.ds(pl.multiple_of(target * part, part), part)
        source, landing = (
            (back_ref.at[:, span], back_in.at[slot]),
            (back_w.at[:, span], back_share.at[slot]),
            (coarse_ref, coarse_in.at[slot]),
            (coarse_w, share_in.at[slot]),
            (scale_in.at[slot], scale_in.at[slot]),
        )[kind]
        return remote(source, landing, meta_send.at[kind, target], meta_recv.at[kind, slot], target, lon)

    def wait_meta(kinds):
        @pl.loop(1, planes)
        def _(k):
            source = lax.rem(lat + k, planes)
            for kind in kinds:
                meta_copy(kind, source, source).wait_recv()

    def chain_copy(kind, upward, unit):
        out, landing, way = (up_out, up_in, 0) if upward else (down_out, down_in, 1)
        target = lat + 1 if upward else lat - 1
        piece, spot = out.at[kind, unit], landing.at[kind, unit]
        return remote(piece, spot, chain_send.at[kind, way, unit], chain_recv.at[kind, way, unit], target, lon)

    def chain_begin(kind, unit):
        if planes == 1:
            return

        @pl.when(lat == 0)
        def _():
            up_out[kind, unit] = own[kind, unit].astype(jnp.bfloat16)
            chain_copy(kind, True, unit).start()

        @pl.when(lat == planes - 1)
        def _():
            down_out[kind, unit] = own[kind, unit].astype(jnp.bfloat16)
            chain_copy(kind, False, unit).start()

    def chain_hop(kind, hop, unit):
        @pl.when((lat == hop) & (unit >= 0) & (unit < units))
        def _():
            chain_copy(kind, True, unit).wait_recv()
            up_out[kind, unit] = (own[kind, unit].astype(jnp.float32) + up_in[kind, unit].astype(jnp.float32)).astype(jnp.bfloat16)
            chain_copy(kind, True, unit).start()

        @pl.when((lat == planes - 1 - hop) & (unit >= 0) & (unit < units))
        def _():
            chain_copy(kind, False, unit).wait_recv()
            down_out[kind, unit] = (own[kind, unit].astype(jnp.float32) + down_in[kind, unit].astype(jnp.float32)).astype(jnp.bfloat16)
            chain_copy(kind, False, unit).start()

    def chain_late(kind, unit):
        for hop in range(2, planes - 1):
            chain_hop(kind, hop, unit)

    def chain_early(kind, unit):
        if planes > 2:
            chain_hop(kind, 1, unit)

    def chain_ready(kind, unit):
        if planes == 1:
            return

        @pl.when(lat == 0)
        def _():
            chain_copy(kind, False, unit).wait_recv()

        @pl.when(lat == planes - 1)
        def _():
            chain_copy(kind, True, unit).wait_recv()

    def chain_total(kind, unit):
        ends = up_in[kind, unit].astype(jnp.float32) + down_in[kind, unit].astype(jnp.float32)
        return own[kind, unit].astype(jnp.float32) + ends

    def chain_sent(kind):
        @pl.loop(0, units)
        def _(unit):
            @pl.when(lat < planes - 1)
            def _():
                chain_copy(kind, True, unit).wait_send()

            @pl.when(lat > 0)
            def _():
                chain_copy(kind, False, unit).wait_send()

    def sub_rows(step):
        return pl.ds(pl.multiple_of(step * BLOCK, BLOCK), BLOCK)

    barrier = pltpu.get_barrier_semaphore()
    for k in range(1, lon_count):
        pl.semaphore_signal(
            barrier, inc=1, device_id=(lat, lax.rem(lon + k, lon_count)), device_id_type=pl.DeviceIdType.MESH
        )
    for k in range(1, planes):
        pl.semaphore_signal(
            barrier, inc=1, device_id=(lax.rem(lat + k, planes), lon), device_id_type=pl.DeviceIdType.MESH
        )
    tabs[lon, groups[0]] = lw_ref[...]
    tabs[lon, groups[1]] = sw_ref[...]
    scale_in[lat, pl.ds(0, lw_count)] = lw_scale[...]
    scale_in[lat, pl.ds(lw_count, band_count - lw_count)] = sw_scale[...] * sun_ref[...].astype(jnp.float32)
    scale_in[lat, pl.ds(band_count, scale_in.shape[1] - band_count)] = jnp.zeros(
        (scale_in.shape[1] - band_count, row_count), jnp.float32
    )
    span = pl.ds(pl.multiple_of(lat * part, part), part)
    back_in[lat] = back_ref[:, span]
    back_share[lat] = back_w[:, span]
    coarse_in[lat] = coarse_ref[...]
    share_in[lat] = coarse_w[...]
    stacked[:, pl.ds(0, width)] = cot_ref[...]
    for v in range(var_count):
        stacked[:, pl.ds((v + 1) * width, width)] = inc_ref[v]

    @pl.when(lat == 0)
    def _():
        up_in[...] = jnp.zeros_like(up_in)

    @pl.when(lat == planes - 1)
    def _():
        down_in[...] = jnp.zeros_like(down_in)

    pl.semaphore_wait(barrier, lon_count + planes - 2)
    table_start(0)
    for kinds in ((0, 1), (2, 3, 4)):
        for k in range(1, planes):
            for kind in kinds:
                meta_copy(kind, lax.rem(lat + k, planes), lat).start()

    @pl.loop(0, planes)
    def _(block):
        rows = pl.ds(pl.multiple_of(block * part, part), part)
        table = pick(column_of(perm_ref[:, rows]) == lane_iota(part, col_count))
        moved = dot(table, stacked[...]).astype(jnp.bfloat16)
        cot_out[block] = moved[:, :width].reshape(lon_count, segment, width)
        fields_out[block] = moved[:, width:].reshape(lon_count, segment, flat_width)
        start_block(0, cot_out, cot_in, block)

    table_relay(0)
    table_start(1)
    start_block(1, fields_out, fields_in, 0)

    wait_meta((0, 1))

    @pl.loop(0, planes)
    def _(block):
        spot = lane_iota(part, row_count)
        first, second = column_of(back_in[block, 0:1, :]), column_of(back_in[block, 1:2, :])
        btab[block] = blend(first == spot, second == spot, column_of(back_share[block]))

    @pl.loop(0, planes)
    def _(block):
        wait_block(0, cot_in, block)
        partial = dot(jnp.transpose(cot_in[block].reshape(part, width)), btab[block])
        for step in range(row_blocks):
            own[0, block * row_blocks + step] = partial[:, step * BLOCK : (step + 1) * BLOCK].astype(own.dtype)
            chain_begin(0, block * row_blocks + step)

    def build(group):
        depth = lw_ref.shape[2]
        for b in range(lw_count) if group == 0 else range(lw_count, band_count):
            for v in range(var_count):
                piece = tabs[:, b, v].reshape(lon_count * depth, width)
                wide[pl.ds(v * lon_count * depth, lon_count * depth), pl.ds(b * width, width)] = piece
                turned[pl.ds(b * width, width), pl.ds(v * lon_count * depth, lon_count * depth)] = jnp.transpose(piece)

    table_finish(0)

    table_relay(1)

    @pl.loop(1, planes)
    def _(block):
        start_block(1, fields_out, fields_in, block)

    table_wait(0)
    build(0)

    @pl.loop(0, row_blocks)
    def _(unit):
        chain_early(0, unit)

    table_finish(1)
    table_wait(1)

    build(1)

    wait_meta((2, 3, 4))

    @pl.loop(0, planes + 3)
    def _(turn):
        @pl.when(turn < planes)
        def _():
            block = turn
            wait_block(1, fields_in, block)
            fields_t[...] = jnp.transpose(fields_in[block].reshape(part, flat_width))

            @pl.loop(0, row_blocks)
            def _(step):
                unit = block * row_blocks + step
                rows = sub_rows(step)
                spot = row_iota(part, BLOCK, lat * part)
                index = coarse_in[block, :, rows]
                table = blend(index[0:1, :] == spot, index[1:2, :] == spot, share_in[block, :, rows])
                ctab[block, :, rows] = table
                coarse = dot(fields_t[...], table).astype(jnp.bfloat16)
                scale = scale_in[block, :, rows]
                total = jnp.zeros((width, BLOCK), jnp.float32)
                for start in range(0, band_count, BUNCH):
                    stop = min(start + BUNCH, band_count)
                    bunch = dot(turned[start * width : stop * width, :], coarse)
                    for b in range(start, stop):
                        total = total + scale[b : b + 1, :] * bunch[(b - start) * width : (b - start + 1) * width, :]
                own[1, unit] = total.astype(own.dtype)
                chain_begin(1, unit)
                chain_early(0, unit + row_blocks)
                chain_late(0, unit)
                chain_late(1, unit - 2 * row_blocks)

        @pl.when(turn >= 3)
        def _():
            block = turn - 3
            for step in range(row_blocks):
                unit = block * row_blocks + step
                chain_ready(1, unit)
                heat[pl.ds(step * BLOCK, BLOCK), :] = jnp.transpose(chain_total(1, unit)).astype(jnp.bfloat16)
            moved = dot(btab[block], heat[...]).astype(jnp.bfloat16)
            tend_out[block] = moved.reshape(lon_count, segment, width)
            start_block(3, tend_out, result_in.at[:, :, :, pl.ds(0, width)], block)

        @pl.when((turn >= 1) & (turn <= planes))
        def _():
            block = turn - 1

            @pl.loop(0, row_blocks)
            def _(step):
                unit = block * row_blocks + step
                chain_ready(0, unit)
                rows = sub_rows(step)
                coarse = chain_total(0, unit)
                scale = scale_in[block, :, rows]
                lifted = jnp.concatenate(
                    [(scale[b : b + 1, :] * coarse).astype(jnp.bfloat16) for b in range(band_count)], axis=0
                )
                adj[:, rows] = dot(wide[...], lifted).astype(jnp.bfloat16)
                if planes > 2:

                    @pl.when(block == 0)
                    def _():
                        chain_hop(1, 1, unit)

                    chain_hop(1, 1, unit + row_blocks)

                    @pl.when(block >= planes - 2)
                    def _():
                        chain_late(1, unit)

            moved = lax.dot_general(ctab[block], adj[...], (((1,), (1,)), ((), ())), preferred_element_type=jnp.float32)
            grad_out[block] = moved.astype(jnp.bfloat16).reshape(lon_count, segment, flat_width)
            start_block(2, grad_out, result_in.at[:, :, :, pl.ds(width, flat_width)], block)

    for group in range(2):
        table_sent(group)

    @pl.loop(1, planes)
    def _(k):
        for kind in range(5):
            meta_copy(kind, lax.rem(lat + k, planes), lat).wait_send()

    chain_sent(0)
    chain_sent(1)
    wait_sent(0, cot_out)
    wait_sent(1, fields_out)

    @pl.loop(0, planes)
    def _(block):
        wait_block(2, result_in.at[:, :, :, pl.ds(width, flat_width)], block)
        wait_block(3, result_in.at[:, :, :, pl.ds(0, width)], block)

    wait_sent(2, grad_out)
    wait_sent(3, tend_out)


def restore_kernel(perm_ref, result_ref, tend_done, grad_done):
    rows, width = tend_done.shape
    col_count = result_ref.shape[0]
    table = pick(perm_ref[...] == row_iota(rows, col_count, pl.program_id(0) * rows))
    moved = dot(table, result_ref[...]).astype(jnp.bfloat16)
    tend_done[...] = moved[:, :width]
    for v in range(grad_done.shape[0]):
        grad_done[v] = moved[:, (v + 1) * width : (v + 2) * width]


def local(
    increments,
    cotangent,
    owner_perm,
    coarse_index,
    coarse_weight,
    back_index,
    back_weight,
    lw_scale,
    sw_scale,
    sunlit,
    lw_table,
    sw_table,
    *,
    planes,
    lon_count,
):
    col_count, var_count, width = increments.shape
    row_count = coarse_weight.shape[0]
    segment = col_count // (planes * lon_count)
    part = lon_count * segment
    flat_width = var_count * width
    thin, thick = (planes, lon_count, segment, width), (planes, lon_count, segment, flat_width)
    bands = lw_table.shape[0] + sw_table.shape[0]
    scale_rows = -(-(bands + 1) // 8) * 8
    wire = (2, planes * (row_count // BLOCK), width, BLOCK)
    half, full, whole = jnp.bfloat16, jnp.float32, jnp.int32
    vmem = pl.BlockSpec(memory_space=pltpu.VMEM)
    scratch = [
        ((col_count, (var_count + 1) * width), half),
        (thin, half),
        (thin, half),
        (thick, half),
        (thick, half),
        (thick, half),
        (thin, half),
        ((lon_count, bands) + lw_table.shape[1:], half),
        ((flat_width, bands * width), half),
        ((bands * width, flat_width), half),
        ((planes, part, row_count), half),
        ((planes, part, row_count), half),
        ((flat_width, part), half),
        ((flat_width, row_count), half),
        ((row_count, width), half),
        (wire, half),
        (wire, half),
        (wire, half),
        (wire, half),
        (wire, full if planes * row_count <= WIDE_SUMS else half),
        ((planes, scale_rows, row_count), full),
        ((planes, 2, row_count), whole),
        ((planes, 1, row_count), full),
        ((planes, 2, part), whole),
        ((planes, 1, part), full),
    ]
    units = planes * (row_count // BLOCK)
    sems = (
        (4, planes, lon_count),
        (4, planes, lon_count),
        (2, 2, units),
        (2, 2, units),
        (5, planes),
        (5, planes),
        (2, lon_count // 2 + 2, lon_count),
        (2, lon_count),
    )
    stack_width = (var_count + 1) * width
    args = (
        owner_perm,
        jnp.transpose(increments, (1, 0, 2)),
        cotangent,
        back_index,
        back_weight[None, :],
        lw_scale,
        sw_scale,
        sunlit[None, :],
        lw_table,
        sw_table,
        coarse_index,
        coarse_weight[None, :],
    )
    received = pl.pallas_call(
        radiate_kernel,
        out_shape=jax.ShapeDtypeStruct((planes, lon_count, segment, stack_width), half),
        in_specs=[vmem] * len(args),
        out_specs=vmem,
        scratch_shapes=[pltpu.VMEM(shape, kind) for shape, kind in scratch]
        + [pltpu.SemaphoreType.DMA(shape) for shape in sems],
        compiler_params=pltpu.CompilerParams(
            vmem_limit_bytes=62 * 1024 * 1024, has_side_effects=True, collective_id=0
        ),
        cost_estimate=pl.CostEstimate(
            flops=12 * planes * row_count * bands * flat_width * width, bytes_accessed=4 << 20, transcendentals=0
        ),
    )(*args)
    steps = col_count // FINAL
    tendency, gradient = pl.pallas_call(
        restore_kernel,
        grid=(steps,),
        out_shape=[
            jax.ShapeDtypeStruct((col_count, width), half),
            jax.ShapeDtypeStruct((var_count, col_count, width), half),
        ],
        in_specs=[
            pl.BlockSpec((1, col_count), lambda i: (0, 0)),
            pl.BlockSpec((col_count, stack_width), lambda i: (0, 0)),
        ],
        out_specs=[
            pl.BlockSpec((FINAL, width), lambda i: (i, 0)),
            pl.BlockSpec((var_count, FINAL, width), lambda i: (0, i, 0)),
        ],
        compiler_params=pltpu.CompilerParams(vmem_limit_bytes=32 * 1024 * 1024),
        cost_estimate=pl.CostEstimate(
            flops=2 * col_count * col_count * stack_width, bytes_accessed=4 << 20, transcendentals=0
        ),
    )(owner_perm, received.reshape(col_count, stack_width))
    return (tendency, jnp.transpose(gradient, (1, 0, 2)))


def solution(mesh):
    in_specs = (
        P(("lat", "lon"), None, None),
        P(("lat", "lon"), None),
        P(("lat", "lon"), None),
        P(None, ("lat", "lon")),
        P(("lat", "lon")),
        P(None, ("lat", "lon")),
        P(("lat", "lon")),
        P(None, ("lat", "lon")),
        P(None, ("lat", "lon")),
        P(("lat", "lon")),
        P(None, None, "lon", None),
        P(None, None, "lon", None),
    )
    out_specs = (P(("lat", "lon"), None), P(("lat", "lon"), None, None))

    def body(*args):
        return local(*args, planes=mesh.shape["lat"], lon_count=mesh.shape["lon"])

    return jax.shard_map(body, mesh=mesh, in_specs=in_specs, out_specs=out_specs, check_vma=False)
```

```python
import jax
import jax.numpy as jnp
from jax import lax
from jax.experimental import pallas as pl
from jax.experimental.pallas import tpu as pltpu
from jax.sharding import PartitionSpec as P

BLOCK = 256
FINAL = 512
BUNCH = 3
WIDE_SUMS = 4096


def lane_iota(rows, width):
    return lax.broadcasted_iota(jnp.int32, (rows, width), 1)


def row_iota(rows, width, start):
    return lax.broadcasted_iota(jnp.int32, (rows, width), 0) + start


def pick(hit):
    return jnp.where(hit, 1.0, 0.0).astype(jnp.bfloat16)


def blend(hit_first, hit_second, share):
    first = jnp.where(hit_first, share, 0.0)
    second = jnp.where(hit_second, 1.0 - share, 0.0)
    return (first + second).astype(jnp.bfloat16)


def dot(left, right):
    return lax.dot_general(left, right, (((1,), (0,)), ((), ())), preferred_element_type=jnp.float32)


def column_of(values):
    return jnp.transpose(jnp.broadcast_to(values, (8, values.shape[1])))[:, 0:1]


def radiate_kernel(
    perm_ref,
    inc_ref,
    cot_ref,
    back_ref,
    back_w,
    lw_scale,
    sw_scale,
    sun_ref,
    lw_ref,
    sw_ref,
    coarse_ref,
    coarse_w,
    result_in,
    stacked,
    cot_out,
    cot_in,
    fields_out,
    fields_in,
    grad_out,
    tend_out,
    tabs,
    wide,
    turned,
    ctab,
    btab,
    fields_t,
    kept,
    adj,
    heat,
    up_out,
    up_in,
    down_out,
    down_in,
    own,
    scale_in,
    coarse_in,
    share_in,
    back_in,
    back_share,
    send_sem,
    recv_sem,
    chain_send,
    chain_recv,
    meta_send,
    meta_recv,
    tab_send,
    tab_recv,
    keep_sem,
):
    var_count, col_count, width = inc_ref.shape
    planes, lon_count, segment = cot_out.shape[0], cot_out.shape[1], cot_out.shape[2]
    part = lon_count * segment
    row_count = lw_scale.shape[1]
    lw_count = lw_ref.shape[0]
    band_count = lw_count + sw_ref.shape[0]
    flat_width = var_count * width
    row_blocks = row_count // BLOCK
    units = planes * row_blocks
    lat, lon = lax.axis_index("lat"), lax.axis_index("lon")
    parity = lax.rem(lon, 2)
    partner = lon + 1 - 2 * parity
    lw_half, sw_half = lw_count // 2, lw_count + (band_count - lw_count) // 2
    edges = (0, lw_half, lw_count, sw_half, band_count)
    groups = tuple(pl.ds(edges[i], edges[i + 1] - edges[i]) for i in range(4))

    def remote(source, landing, send, recv, target_lat, target_lon):
        return pltpu.make_async_remote_copy(
            src_ref=source,
            dst_ref=landing,
            send_sem=send,
            recv_sem=recv,
            device_id=(target_lat, target_lon),
            device_id_type=pl.DeviceIdType.MESH,
        )

    def table_copy(group, slot, target):
        piece = tabs.at[slot, groups[group]]
        return remote(piece, piece, tab_send.at[group], tab_recv.at[group, slot], lat, target)

    quad = lon_count == 8
    if quad:
        across = lon + 2 - 4 * lax.rem(lax.div(lon, 2), 2)
        along = lon + 4 - 8 * lax.div(lon, 4)
        near, far = (across, along), across + along - lon
    else:
        near, far = tuple(lax.rem(lon + 2 * j, lon_count) for j in range(1, lon_count // 2)), None

    def relay(group):
        return table_copy(group, near[group % 2], near[1 - group % 2])

    def table_start(half):
        for group in (2 * half, 2 * half + 1):
            for target in near + (partner,):
                table_copy(group, lon, target).start()

    def table_relay(half):
        for group in (2 * half, 2 * half + 1):
            for source in near:
                table_copy(group, source, source).wait_recv()
            if quad:
                relay(group).start()
            for source in near:
                table_copy(group, source, partner).start()

    def table_finish(half):
        if quad:
            for group in (2 * half, 2 * half + 1):
                table_copy(group, far, far).wait_recv()
                table_copy(group, far, partner).start()

    def table_wait(half):
        for group in (2 * half, 2 * half + 1):
            for j in range(lon_count // 2):
                source = lax.rem(partner + 2 * j, lon_count)
                table_copy(group, source, source).wait_recv()

    def table_sent(group):
        pieces = tabs.at[pl.ds(0, lon_count - 1), groups[group]]
        remote(pieces, pieces, tab_send.at[group], tab_recv.at[group, 0], lat, partner).wait_send()

    def copy(kind, source, landing, block, target):
        return remote(source, landing, send_sem.at[kind], recv_sem.at[kind, block], lat, target)

    def keep_copy(kind, source, landing, block):
        return pltpu.make_async_copy(source.at[block, lon], landing.at[block, lon], keep_sem.at[kind - 2])

    def start_block(kind, source, landing, block):
        if kind < 2:
            landing[block, lon] = source[block, lon]
        else:
            keep_copy(kind, source, landing, block).start()

        @pl.loop(1, lon_count)
        def _(k):
            target = lax.rem(lon + k, lon_count)
            copy(kind, source.at[block, target], landing.at[block, lon], block, target).start()

    def wait_block(kind, landing, block):
        pieces = landing.at[block, pl.ds(0, lon_count - 1)]
        copy(kind, pieces, pieces, block, partner).wait_recv()

    def wait_sent(kind, source):
        pieces = source.at[:, pl.ds(0, lon_count - 1)]
        copy(kind, pieces, pieces, 0, partner).wait_send()

    def meta_copy(kind, target, slot):
        span = pl.ds(pl.multiple_of(target * part, part), part)
        source, landing = (
            (back_ref.at[:, span], back_in.at[slot]),
            (back_w.at[:, span], back_share.at[slot]),
            (coarse_ref, coarse_in.at[slot]),
            (coarse_w, share_in.at[slot]),
            (scale_in.at[slot], scale_in.at[slot]),
        )[kind]
        return remote(source, landing, meta_send.at[kind], meta_recv.at[kind], target, lon)

    def meta_whole(kind):
        pieces = (back_in, back_share, coarse_in, share_in, scale_in)[kind].at[pl.ds(0, planes - 1)]
        return remote(pieces, pieces, meta_send.at[kind], meta_recv.at[kind], lat, partner)

    def wait_meta(kinds):
        if planes > 1:
            for kind in kinds:
                meta_whole(kind).wait_recv()

    def chain_copy(kind, upward, unit):
        out, landing, way = (up_out, up_in, 0) if upward else (down_out, down_in, 1)
        target = lat + 1 if upward else lat - 1
        piece, spot = out.at[kind, unit], landing.at[kind, unit]
        return remote(piece, spot, chain_send.at[kind, way], chain_recv.at[kind, way, unit], target, lon)

    def chain_begin(kind, unit):
        if planes == 1:
            return

        @pl.when(lat == 0)
        def _():
            up_out[kind, unit] = own[kind, unit].astype(jnp.bfloat16)
            chain_copy(kind, True, unit).start()

        @pl.when(lat == planes - 1)
        def _():
            down_out[kind, unit] = own[kind, unit].astype(jnp.bfloat16)
            chain_copy(kind, False, unit).start()

    def chain_hop(kind, hop, unit):
        @pl.when((lat == hop) & (unit >= 0) & (unit < units))
        def _():
            chain_copy(kind, True, unit).wait_recv()
            up_out[kind, unit] = (own[kind, unit].astype(jnp.float32) + up_in[kind, unit].astype(jnp.float32)).astype(jnp.bfloat16)
            chain_copy(kind, True, unit).start()

        @pl.when((lat == planes - 1 - hop) & (unit >= 0) & (unit < units))
        def _():
            chain_copy(kind, False, unit).wait_recv()
            down_out[kind, unit] = (own[kind, unit].astype(jnp.float32) + down_in[kind, unit].astype(jnp.float32)).astype(jnp.bfloat16)
            chain_copy(kind, False, unit).start()

    def chain_late(kind, unit):
        for hop in range(2, planes - 1):
            chain_hop(kind, hop, unit)

    def chain_early(kind, unit):
        if planes > 2:
            chain_hop(kind, 1, unit)

    def chain_ready(kind, unit):
        if planes == 1:
            return

        @pl.when(lat == 0)
        def _():
            chain_copy(kind, False, unit).wait_recv()

        @pl.when(lat == planes - 1)
        def _():
            chain_copy(kind, True, unit).wait_recv()

    def chain_total(kind, unit):
        ends = up_in[kind, unit].astype(jnp.float32) + down_in[kind, unit].astype(jnp.float32)
        return own[kind, unit].astype(jnp.float32) + ends

    def chain_sent(kind):
        @pl.when(lat < planes - 1)
        def _():
            pieces = up_out.at[kind]
            remote(pieces, pieces, chain_send.at[kind, 0], chain_recv.at[kind, 0, 0], lat, partner).wait_send()

        @pl.when(lat > 0)
        def _():
            pieces = down_out.at[kind]
            remote(pieces, pieces, chain_send.at[kind, 1], chain_recv.at[kind, 1, 0], lat, partner).wait_send()

    def sub_rows(step):
        return pl.ds(pl.multiple_of(step * BLOCK, BLOCK), BLOCK)

    barrier = pltpu.get_barrier_semaphore()
    for k in range(1, lon_count):
        pl.semaphore_signal(
            barrier, inc=1, device_id=(lat, lax.rem(lon + k, lon_count)), device_id_type=pl.DeviceIdType.MESH
        )
    for k in range(1, planes):
        pl.semaphore_signal(
            barrier, inc=1, device_id=(lax.rem(lat + k, planes), lon), device_id_type=pl.DeviceIdType.MESH
        )
    tabs[lon, pl.ds(0, lw_count)] = lw_ref[...]
    tabs[lon, pl.ds(lw_count, band_count - lw_count)] = sw_ref[...]
    scale_in[lat, pl.ds(0, lw_count)] = lw_scale[...]
    scale_in[lat, pl.ds(lw_count, band_count - lw_count)] = sw_scale[...] * sun_ref[...].astype(jnp.float32)
    scale_in[lat, pl.ds(band_count, scale_in.shape[1] - band_count)] = jnp.zeros(
        (scale_in.shape[1] - band_count, row_count), jnp.float32
    )
    span = pl.ds(pl.multiple_of(lat * part, part), part)
    back_in[lat] = back_ref[:, span]
    back_share[lat] = back_w[:, span]
    coarse_in[lat] = coarse_ref[...]
    share_in[lat] = coarse_w[...]
    stacked[:, pl.ds(0, width)] = cot_ref[...]
    for v in range(var_count):
        stacked[:, pl.ds((v + 1) * width, width)] = inc_ref[v]

    @pl.when(lat == 0)
    def _():
        up_in[...] = jnp.zeros_like(up_in)

    @pl.when(lat == planes - 1)
    def _():
        down_in[...] = jnp.zeros_like(down_in)

    pl.semaphore_wait(barrier, lon_count + planes - 2)
    table_start(0)
    for kinds in ((0, 1), (2, 3, 4)):
        for k in range(1, planes):
            for kind in kinds:
                meta_copy(kind, lax.rem(lat + k, planes), lat).start()

    @pl.loop(0, planes)
    def _(block):
        rows = pl.ds(pl.multiple_of(block * part, part), part)
        table = pick(column_of(perm_ref[:, rows]) == lane_iota(part, col_count))
        moved = dot(table, stacked[...]).astype(jnp.bfloat16)
        cot_out[block] = moved[:, :width].reshape(lon_count, segment, width)
        fields_out[block] = moved[:, width:].reshape(lon_count, segment, flat_width)
        start_block(0, cot_out, cot_in, block)

    table_relay(0)
    start_block(1, fields_out, fields_in, 0)
    table_start(1)

    wait_meta((0, 1))

    @pl.loop(0, planes)
    def _(block):
        spot = lane_iota(part, row_count)
        first, second = column_of(back_in[block, 0:1, :]), column_of(back_in[block, 1:2, :])
        btab[block] = blend(first == spot, second == spot, column_of(back_share[block]))

    @pl.loop(0, planes)
    def _(block):
        wait_block(0, cot_in, block)
        partial = dot(jnp.transpose(cot_in[block].reshape(part, width)), btab[block])
        for step in range(row_blocks):
            own[0, block * row_blocks + step] = partial[:, step * BLOCK : (step + 1) * BLOCK].astype(own.dtype)
            chain_begin(0, block * row_blocks + step)

    def build(group):
        depth = lw_ref.shape[2]
        for b in range(lw_count) if group == 0 else range(lw_count, band_count):
            for v in range(var_count):
                piece = tabs[:, b, v].reshape(lon_count * depth, width)
                wide[pl.ds(v * lon_count * depth, lon_count * depth), pl.ds(b * width, width)] = piece
                turned[pl.ds(b * width, width), pl.ds(v * lon_count * depth, lon_count * depth)] = jnp.transpose(piece)

    def bands(first, last, block, rows, coarse, total):
        scale = scale_in[block, :, rows]
        for start in range(first, last, BUNCH):
            stop = min(start + BUNCH, last)
            bunch = dot(turned[start * width : stop * width, :], coarse)
            for b in range(start, stop):
                total = total + scale[b : b + 1, :] * bunch[(b - start) * width : (b - start + 1) * width, :]
        return total

    def gather_fields(block):
        wait_block(1, fields_in, block)
        fields_t[...] = jnp.transpose(fields_in[block].reshape(part, flat_width))

    def interpolate(block, rows):
        spot = row_iota(part, BLOCK, lat * part)
        index = coarse_in[block, :, rows]
        table = blend(index[0:1, :] == spot, index[1:2, :] == spot, share_in[block, :, rows])
        ctab[block, :, rows] = table
        return dot(fields_t[...], table).astype(jnp.bfloat16)

    table_finish(0)
    table_wait(0)

    build(0)
    wait_meta((2, 3, 4))

    gather_fields(0)

    @pl.loop(0, row_blocks)
    def _(step):
        rows = sub_rows(step)
        coarse = interpolate(0, rows)
        kept[step] = coarse
        own[1, step] = bands(0, lw_count, 0, rows, coarse, jnp.zeros((width, BLOCK), jnp.float32)).astype(own.dtype)
        chain_early(0, step)

    table_relay(1)

    @pl.loop(1, planes)
    def _(block):
        start_block(1, fields_out, fields_in, block)

    @pl.loop(0, row_blocks)
    def _(step):
        chain_early(0, step + row_blocks)
        chain_late(0, step)

    table_finish(1)
    table_wait(1)

    build(1)

    @pl.loop(0, planes)
    def _(turn):
        def follow(unit):
            chain_begin(1, unit)
            chain_early(0, unit + 2 * row_blocks)
            chain_late(0, unit + row_blocks)
            chain_early(1, unit - 2 * row_blocks)
            chain_late(1, unit - 3 * row_blocks)

        @pl.when(turn == 0)
        def _():
            @pl.loop(0, row_blocks)
            def _(step):
                begun = own[1, step].astype(jnp.float32)
                total = bands(lw_count, band_count, 0, sub_rows(step), kept[step], begun)
                own[1, step] = total.astype(own.dtype)
                follow(step)

        @pl.when(turn > 0)
        def _():
            block = turn
            gather_fields(block)

            @pl.loop(0, row_blocks)
            def _(step):
                unit = block * row_blocks + step
                rows = sub_rows(step)
                coarse = interpolate(block, rows)
                zero = jnp.zeros((width, BLOCK), jnp.float32)
                own[1, unit] = bands(0, band_count, block, rows, coarse, zero).astype(own.dtype)
                follow(unit)

    def finish_heat(block):
        for step in range(row_blocks):
            unit = block * row_blocks + step
            chain_ready(1, unit)
            heat[pl.ds(step * BLOCK, BLOCK), :] = jnp.transpose(chain_total(1, unit)).astype(jnp.bfloat16)
        moved = dot(btab[block], heat[...]).astype(jnp.bfloat16)
        tend_out[block] = moved.reshape(lon_count, segment, width)
        start_block(3, tend_out, result_in.at[:, :, :, pl.ds(0, width)], block)

    @pl.loop(0, planes + 1)
    def _(turn):
        @pl.when(turn > 0)
        def _():
            finish_heat(turn - 1)

        @pl.when(turn < planes)
        def _():
            block = turn

            @pl.loop(0, row_blocks)
            def _(step):
                unit = block * row_blocks + step
                chain_ready(0, unit)
                rows = sub_rows(step)
                coarse = chain_total(0, unit)
                scale = scale_in[block, :, rows]
                lifted = jnp.concatenate(
                    [(scale[b : b + 1, :] * coarse).astype(jnp.bfloat16) for b in range(band_count)], axis=0
                )
                adj[:, rows] = dot(wide[...], lifted).astype(jnp.bfloat16)
                chain_early(1, unit + units - 2 * row_blocks)
                chain_late(1, unit + units - 3 * row_blocks)

            moved = lax.dot_general(ctab[block], adj[...], (((1,), (1,)), ((), ())), preferred_element_type=jnp.float32)
            grad_out[block] = moved.astype(jnp.bfloat16).reshape(lon_count, segment, flat_width)
            start_block(2, grad_out, result_in.at[:, :, :, pl.ds(width, flat_width)], block)

    for group in range(4):
        table_sent(group)

    if planes > 1:
        for kind in range(5):
            meta_whole(kind).wait_send()

    chain_sent(0)
    chain_sent(1)
    wait_sent(0, cot_out)
    wait_sent(1, fields_out)

    @pl.loop(0, planes)
    def _(block):
        wait_block(2, result_in.at[:, :, :, pl.ds(width, flat_width)], block)
        wait_block(3, result_in.at[:, :, :, pl.ds(0, width)], block)

    wait_sent(2, grad_out)
    wait_sent(3, tend_out)

    for kind, source, start in ((2, grad_out, width), (3, tend_out, 0)):
        piece = source.at[:, 0]
        kept_piece = result_in.at[:, 0, :, pl.ds(start, source.shape[-1])]
        pltpu.make_async_copy(piece, kept_piece, keep_sem.at[kind - 2]).wait()


def restore_kernel(perm_ref, result_ref, tend_done, grad_done):
    rows, width = tend_done.shape
    col_count = result_ref.shape[0]
    table = pick(perm_ref[...] == row_iota(rows, col_count, pl.program_id(0) * rows))
    moved = dot(table, result_ref[...]).astype(jnp.bfloat16)
    tend_done[...] = moved[:, :width]
    for v in range(grad_done.shape[0]):
        grad_done[v] = moved[:, (v + 1) * width : (v + 2) * width]


def local(
    increments,
    cotangent,
    owner_perm,
    coarse_index,
    coarse_weight,
    back_index,
    back_weight,
    lw_scale,
    sw_scale,
    sunlit,
    lw_table,
    sw_table,
    *,
    planes,
    lon_count,
):
    col_count, var_count, width = increments.shape
    row_count = coarse_weight.shape[0]
    segment = col_count // (planes * lon_count)
    part = lon_count * segment
    flat_width = var_count * width
    thin, thick = (planes, lon_count, segment, width), (planes, lon_count, segment, flat_width)
    bands = lw_table.shape[0] + sw_table.shape[0]
    scale_rows = -(-(bands + 1) // 8) * 8
    wire = (2, planes * (row_count // BLOCK), width, BLOCK)
    half, full, whole = jnp.bfloat16, jnp.float32, jnp.int32
    vmem = pl.BlockSpec(memory_space=pltpu.VMEM)
    scratch = [
        ((col_count, (var_count + 1) * width), half),
        (thin, half),
        (thin, half),
        (thick, half),
        (thick, half),
        (thick, half),
        (thin, half),
        ((lon_count, bands) + lw_table.shape[1:], half),
        ((flat_width, bands * width), half),
        ((bands * width, flat_width), half),
        ((planes, part, row_count), half),
        ((planes, part, row_count), half),
        ((flat_width, part), half),
        ((row_count // BLOCK, flat_width, BLOCK), half),
        ((flat_width, row_count), half),
        ((row_count, width), half),
        (wire, half),
        (wire, half),
        (wire, half),
        (wire, half),
        (wire, full if planes * row_count <= WIDE_SUMS else half),
        ((planes, scale_rows, row_count), full),
        ((planes, 2, row_count), whole),
        ((planes, 1, row_count), full),
        ((planes, 2, part), whole),
        ((planes, 1, part), full),
    ]
    units = planes * (row_count // BLOCK)
    sems = (
        (4,),
        (4, planes),
        (2, 2),
        (2, 2, units),
        (5,),
        (5,),
        (4,),
        (4, lon_count),
        (2,),
    )
    stack_width = (var_count + 1) * width
    args = (
        owner_perm,
        jnp.transpose(increments, (1, 0, 2)),
        cotangent,
        back_index,
        back_weight[None, :],
        lw_scale,
        sw_scale,
        sunlit[None, :],
        lw_table,
        sw_table,
        coarse_index,
        coarse_weight[None, :],
    )
    received = pl.pallas_call(
        radiate_kernel,
        out_shape=jax.ShapeDtypeStruct((planes, lon_count, segment, stack_width), half),
        in_specs=[vmem] * len(args),
        out_specs=pl.BlockSpec(memory_space=pl.ANY),
        scratch_shapes=[pltpu.VMEM(shape, kind) for shape, kind in scratch]
        + [pltpu.SemaphoreType.DMA(shape) for shape in sems],
        compiler_params=pltpu.CompilerParams(
            vmem_limit_bytes=62 * 1024 * 1024, has_side_effects=True, collective_id=0
        ),
        cost_estimate=pl.CostEstimate(
            flops=12 * planes * row_count * bands * flat_width * width, bytes_accessed=4 << 20, transcendentals=0
        ),
    )(*args)
    steps = col_count // FINAL
    tendency, gradient = pl.pallas_call(
        restore_kernel,
        grid=(steps,),
        out_shape=[
            jax.ShapeDtypeStruct((col_count, width), half),
            jax.ShapeDtypeStruct((var_count, col_count, width), half),
        ],
        in_specs=[
            pl.BlockSpec((1, col_count), lambda i: (0, 0)),
            pl.BlockSpec((col_count, stack_width), lambda i: (0, 0)),
        ],
        out_specs=[
            pl.BlockSpec((FINAL, width), lambda i: (i, 0)),
            pl.BlockSpec((var_count, FINAL, width), lambda i: (0, i, 0)),
        ],
        compiler_params=pltpu.CompilerParams(vmem_limit_bytes=32 * 1024 * 1024),
        cost_estimate=pl.CostEstimate(
            flops=2 * col_count * col_count * stack_width, bytes_accessed=4 << 20, transcendentals=0
        ),
    )(owner_perm, received.reshape(col_count, stack_width))
    return (tendency, jnp.transpose(gradient, (1, 0, 2)))


def solution(mesh):
    in_specs = (
        P(("lat", "lon"), None, None),
        P(("lat", "lon"), None),
        P(("lat", "lon"), None),
        P(None, ("lat", "lon")),
        P(("lat", "lon")),
        P(None, ("lat", "lon")),
        P(("lat", "lon")),
        P(None, ("lat", "lon")),
        P(None, ("lat", "lon")),
        P(("lat", "lon")),
        P(None, None, "lon", None),
        P(None, None, "lon", None),
    )
    out_specs = (P(("lat", "lon"), None), P(("lat", "lon"), None, None))

    def body(*args):
        return local(*args, planes=mesh.shape["lat"], lon_count=mesh.shape["lon"])

    return jax.shard_map(body, mesh=mesh, in_specs=in_specs, out_specs=out_specs, check_vma=False)
```

```python
import jax
import jax.numpy as jnp
from jax import lax
from jax.experimental import pallas as pl
from jax.experimental.pallas import tpu as pltpu
from jax.sharding import PartitionSpec as P

BLOCK = 256
FINAL = 512
BUNCH = 3
WIDE_SUMS = 4096
LOADED = (1, 2, 8, 9)


def lane_iota(rows, width):
    return lax.broadcasted_iota(jnp.int32, (rows, width), 1)


def row_iota(rows, width, start):
    return lax.broadcasted_iota(jnp.int32, (rows, width), 0) + start


def pick(hit):
    return jnp.where(hit, 1.0, 0.0).astype(jnp.bfloat16)


def blend(hit_first, hit_second, share):
    first = jnp.where(hit_first, share, 0.0)
    second = jnp.where(hit_second, 1.0 - share, 0.0)
    return (first + second).astype(jnp.bfloat16)


def dot(left, right):
    return lax.dot_general(left, right, (((1,), (0,)), ((), ())), preferred_element_type=jnp.float32)


def column_of(values):
    return jnp.transpose(jnp.broadcast_to(values, (8, values.shape[1])))[:, 0:1]


def radiate_kernel(
    perm_ref,
    inc_ref,
    cot_ref,
    back_ref,
    back_w,
    lw_scale,
    sw_scale,
    sun_ref,
    lw_ref,
    sw_ref,
    coarse_ref,
    coarse_w,
    result_in,
    restored,
    early_in,
    staged,
    stacked,
    cot_out,
    cot_in,
    fields_out,
    fields_in,
    grad_out,
    tend_out,
    tabs,
    wide,
    turned,
    ctab,
    btab,
    fields_t,
    kept,
    adj,
    heat,
    up_out,
    up_in,
    down_out,
    down_in,
    own,
    scale_in,
    coarse_in,
    share_in,
    back_in,
    back_share,
    send_sem,
    recv_sem,
    chain_send,
    chain_recv,
    meta_send,
    meta_recv,
    tab_send,
    tab_recv,
    keep_sem,
    load_sem,
    put_sem,
):
    var_count, col_count, width = inc_ref.shape
    planes, lon_count, segment = cot_out.shape[0], cot_out.shape[1], cot_out.shape[2]
    part = lon_count * segment
    row_count = lw_scale.shape[1]
    lw_count = lw_ref.shape[0]
    band_count = lw_count + sw_ref.shape[0]
    flat_width = var_count * width
    row_blocks = row_count // BLOCK
    units = planes * row_blocks
    half = planes // 2
    early = early_in.shape[0]
    lanes = (pl.ds(width, flat_width), pl.ds(0, width))
    lat, lon = lax.axis_index("lat"), lax.axis_index("lon")
    parity = lax.rem(lon, 2)
    partner = lon + 1 - 2 * parity
    lw_half, sw_half = lw_count // 2, lw_count + (band_count - lw_count) // 2
    edges = (0, lw_half, lw_count, sw_half, band_count)
    groups = tuple(pl.ds(edges[i], edges[i + 1] - edges[i]) for i in range(4))

    def remote(source, landing, send, recv, target_lat, target_lon):
        return pltpu.make_async_remote_copy(
            src_ref=source,
            dst_ref=landing,
            send_sem=send,
            recv_sem=recv,
            device_id=(target_lat, target_lon),
            device_id_type=pl.DeviceIdType.MESH,
        )

    def table_copy(group, slot, target):
        piece = tabs.at[slot, groups[group]]
        return remote(piece, piece, tab_send.at[group], tab_recv.at[group, slot], lat, target)

    quad = lon_count == 8
    if quad:
        across = lon + 2 - 4 * lax.rem(lax.div(lon, 2), 2)
        along = lon + 4 - 8 * lax.div(lon, 4)
        near, far = (across, along), across + along - lon
    else:
        near, far = tuple(lax.rem(lon + 2 * j, lon_count) for j in range(1, lon_count // 2)), None

    def relay(group):
        return table_copy(group, near[group % 2], near[1 - group % 2])

    def table_start(side):
        for group in (2 * side, 2 * side + 1):
            for target in near + (partner,):
                table_copy(group, lon, target).start()

    def table_relay(side):
        for group in (2 * side, 2 * side + 1):
            for source in near:
                table_copy(group, source, source).wait_recv()
            if quad:
                relay(group).start()
            for source in near:
                table_copy(group, source, partner).start()

    def table_finish(side):
        if quad:
            for group in (2 * side, 2 * side + 1):
                table_copy(group, far, far).wait_recv()
                table_copy(group, far, partner).start()

    def table_wait(side):
        for group in (2 * side, 2 * side + 1):
            for j in range(lon_count // 2):
                source = lax.rem(partner + 2 * j, lon_count)
                table_copy(group, source, source).wait_recv()

    def table_sent(group):
        pieces = tabs.at[pl.ds(0, lon_count - 1), groups[group]]
        remote(pieces, pieces, tab_send.at[group], tab_recv.at[group, 0], lat, partner).wait_send()

    def copy(kind, source, landing, block, target):
        return remote(source, landing, send_sem.at[kind], recv_sem.at[kind, block], lat, target)

    def start_block(kind, source, landing, block, spot=None):
        spot = block if spot is None else spot
        landing = landing.at[spot, lon]
        if kind < 2:
            landing[...] = source[block, lon]
        else:
            pltpu.make_async_copy(source.at[block, lon], landing, keep_sem.at[kind - 2]).start()

        @pl.loop(1, lon_count)
        def _(k):
            target = lax.rem(lon + k, lon_count)
            copy(kind, source.at[block, target], landing, block, target).start()

    def return_block(kind, source, block):
        @pl.when(block < early)
        def _():
            start_block(kind, source, early_in.at[:, :, :, lanes[kind - 2]], block)

        @pl.when(block >= early)
        def _():
            start_block(kind, source, result_in.at[:, :, :, lanes[kind - 2]], block, block - early)

    def wait_return(block):
        for kind, landing in ((2, grad_out), (3, tend_out)):
            wait_block(kind, landing, block)

    def wait_block(kind, landing, block):
        pieces = landing.at[block, pl.ds(0, lon_count - 1)]
        copy(kind, pieces, pieces, block, partner).wait_recv()

    def wait_sent(kind, source):
        pieces = source.at[:, pl.ds(0, lon_count - 1)]
        copy(kind, pieces, pieces, 0, partner).wait_send()

    def meta_copy(kind, target, slot):
        span = pl.ds(pl.multiple_of(target * part, part), part)
        source, landing = (
            (back_ref.at[:, span], back_in.at[slot]),
            (back_w.at[:, span], back_share.at[slot]),
            (coarse_ref, coarse_in.at[slot]),
            (coarse_w, share_in.at[slot]),
            (scale_in.at[slot], scale_in.at[slot]),
        )[kind]
        return remote(source, landing, meta_send.at[kind], meta_recv.at[kind], target, lon)

    def meta_whole(kind):
        pieces = (back_in, back_share, coarse_in, share_in, scale_in)[kind].at[pl.ds(0, planes - 1)]
        return remote(pieces, pieces, meta_send.at[kind], meta_recv.at[kind], lat, partner)

    def wait_meta(kinds):
        if planes > 1:
            for kind in kinds:
                meta_whole(kind).wait_recv()

    def chain_copy(kind, upward, unit):
        out, landing, way = (up_out, up_in, 0) if upward else (down_out, down_in, 1)
        target = lat + 1 if upward else lat - 1
        piece, spot = out.at[kind, unit], landing.at[kind, unit]
        return remote(piece, spot, chain_send.at[kind, way], chain_recv.at[kind, way, unit], target, lon)

    def chain_begin(kind, unit):
        if planes == 1:
            return

        @pl.when(lat == 0)
        def _():
            up_out[kind, unit] = own[kind, unit].astype(jnp.bfloat16)
            chain_copy(kind, True, unit).start()

        @pl.when(lat == planes - 1)
        def _():
            down_out[kind, unit] = own[kind, unit].astype(jnp.bfloat16)
            chain_copy(kind, False, unit).start()

    def chain_hop(kind, hop, unit):
        @pl.when((lat == hop) & (unit >= 0) & (unit < units))
        def _():
            chain_copy(kind, True, unit).wait_recv()
            up_out[kind, unit] = (own[kind, unit].astype(jnp.float32) + up_in[kind, unit].astype(jnp.float32)).astype(jnp.bfloat16)
            chain_copy(kind, True, unit).start()

        @pl.when((lat == planes - 1 - hop) & (unit >= 0) & (unit < units))
        def _():
            chain_copy(kind, False, unit).wait_recv()
            down_out[kind, unit] = (own[kind, unit].astype(jnp.float32) + down_in[kind, unit].astype(jnp.float32)).astype(jnp.bfloat16)
            chain_copy(kind, False, unit).start()

    def chain_late(kind, unit):
        for hop in range(2, planes - 1):
            chain_hop(kind, hop, unit)

    def chain_early(kind, unit):
        if planes > 2:
            chain_hop(kind, 1, unit)

    def chain_ready(kind, unit):
        if planes == 1:
            return

        @pl.when(lat == 0)
        def _():
            chain_copy(kind, False, unit).wait_recv()

        @pl.when(lat == planes - 1)
        def _():
            chain_copy(kind, True, unit).wait_recv()

    def chain_total(kind, unit):
        ends = up_in[kind, unit].astype(jnp.float32) + down_in[kind, unit].astype(jnp.float32)
        return own[kind, unit].astype(jnp.float32) + ends

    def chain_sent(kind):
        @pl.when(lat < planes - 1)
        def _():
            pieces = up_out.at[kind]
            remote(pieces, pieces, chain_send.at[kind, 0], chain_recv.at[kind, 0, 0], lat, partner).wait_send()

        @pl.when(lat > 0)
        def _():
            pieces = down_out.at[kind]
            remote(pieces, pieces, chain_send.at[kind, 1], chain_recv.at[kind, 1, 0], lat, partner).wait_send()

    def sub_rows(step):
        return pl.ds(pl.multiple_of(step * BLOCK, BLOCK), BLOCK)

    barrier = pltpu.get_barrier_semaphore()
    for k in range(1, lon_count):
        pl.semaphore_signal(
            barrier, inc=1, device_id=(lat, lax.rem(lon + k, lon_count)), device_id_type=pl.DeviceIdType.MESH
        )
    for k in range(1, planes):
        pl.semaphore_signal(
            barrier, inc=1, device_id=(lax.rem(lat + k, planes), lon), device_id_type=pl.DeviceIdType.MESH
        )
    loads = [
        pltpu.make_async_copy(lw_ref, tabs.at[lon, pl.ds(0, lw_count)], load_sem.at[0]),
        pltpu.make_async_copy(sw_ref, tabs.at[lon, pl.ds(lw_count, band_count - lw_count)], load_sem.at[1]),
        pltpu.make_async_copy(cot_ref, stacked.at[:, pl.ds(0, width)], load_sem.at[2]),
    ] + [
        pltpu.make_async_copy(inc_ref.at[v], stacked.at[:, pl.ds((v + 1) * width, width)], load_sem.at[3 + v])
        for v in range(var_count)
    ]
    for load in loads:
        load.start()
    scale_in[lat, pl.ds(0, lw_count)] = lw_scale[...]
    scale_in[lat, pl.ds(lw_count, band_count - lw_count)] = sw_scale[...] * sun_ref[...].astype(jnp.float32)
    scale_in[lat, pl.ds(band_count, scale_in.shape[1] - band_count)] = jnp.zeros(
        (scale_in.shape[1] - band_count, row_count), jnp.float32
    )
    span = pl.ds(pl.multiple_of(lat * part, part), part)
    back_in[lat] = back_ref[:, span]
    back_share[lat] = back_w[:, span]
    coarse_in[lat] = coarse_ref[...]
    share_in[lat] = coarse_w[...]

    @pl.when(lat == 0)
    def _():
        up_in[...] = jnp.zeros_like(up_in)

    @pl.when(lat == planes - 1)
    def _():
        down_in[...] = jnp.zeros_like(down_in)

    loads[0].wait()
    loads[1].wait()

    pl.semaphore_wait(barrier, lon_count + planes - 2)
    table_start(0)
    for kinds in ((0, 1), (2, 3, 4)):
        for k in range(1, planes):
            for kind in kinds:
                meta_copy(kind, lax.rem(lat + k, planes), lat).start()

    for load in loads[2:]:
        load.wait()

    @pl.loop(0, planes)
    def _(block):
        rows = pl.ds(pl.multiple_of(block * part, part), part)
        table = pick(column_of(perm_ref[:, rows]) == lane_iota(part, col_count))
        moved = dot(table, stacked[...]).astype(jnp.bfloat16)
        cot_out[block] = moved[:, :width].reshape(lon_count, segment, width)
        fields_out[block] = moved[:, width:].reshape(lon_count, segment, flat_width)

        @pl.when(block < half)
        def _():
            start_block(0, cot_out, cot_in, block)

    table_relay(0)
    start_block(1, fields_out, fields_in, 0)
    table_start(1)

    @pl.loop(half, planes)
    def _(block):
        start_block(0, cot_out, cot_in, block)

    wait_meta((0, 1))

    @pl.loop(0, planes)
    def _(block):
        spot = lane_iota(part, row_count)
        first, second = column_of(back_in[block, 0:1, :]), column_of(back_in[block, 1:2, :])
        btab[block] = blend(first == spot, second == spot, column_of(back_share[block]))

    def column_sums(block):
        wait_block(0, cot_in, block)
        partial = dot(jnp.transpose(cot_in[block].reshape(part, width)), btab[block])
        for step in range(row_blocks):
            own[0, block * row_blocks + step] = partial[:, step * BLOCK : (step + 1) * BLOCK].astype(own.dtype)
            chain_begin(0, block * row_blocks + step)

    @pl.loop(0, half)
    def _(block):
        column_sums(block)

    def build(group):
        depth = lw_ref.shape[2]
        for b in range(lw_count) if group == 0 else range(lw_count, band_count):
            for v in range(var_count):
                piece = tabs[:, b, v].reshape(lon_count * depth, width)
                wide[pl.ds(v * lon_count * depth, lon_count * depth), pl.ds(b * width, width)] = piece
                turned[pl.ds(b * width, width), pl.ds(v * lon_count * depth, lon_count * depth)] = jnp.transpose(piece)

    def bands(first, last, block, rows, coarse, total):
        scale = scale_in[block, :, rows]
        for start in range(first, last, BUNCH):
            stop = min(start + BUNCH, last)
            bunch = dot(turned[start * width : stop * width, :], coarse)
            for b in range(start, stop):
                total = total + scale[b : b + 1, :] * bunch[(b - start) * width : (b - start + 1) * width, :]
        return total

    def gather_fields(block):
        wait_block(1, fields_in, block)
        fields_t[...] = jnp.transpose(fields_in[block].reshape(part, flat_width))

    def interpolate(block, rows):
        spot = row_iota(part, BLOCK, lat * part)
        index = coarse_in[block, :, rows]
        table = blend(index[0:1, :] == spot, index[1:2, :] == spot, share_in[block, :, rows])
        ctab[block, :, rows] = table
        return dot(fields_t[...], table).astype(jnp.bfloat16)

    table_finish(0)
    table_wait(0)

    build(0)
    wait_meta((2, 3, 4))

    gather_fields(0)

    @pl.loop(0, row_blocks)
    def _(step):
        rows = sub_rows(step)
        coarse = interpolate(0, rows)
        kept[step] = coarse
        own[1, step] = bands(0, lw_count, 0, rows, coarse, jnp.zeros((width, BLOCK), jnp.float32)).astype(own.dtype)

    table_relay(1)

    @pl.loop(1, planes)
    def _(block):
        start_block(1, fields_out, fields_in, block)

    @pl.loop(0, row_blocks)
    def _(step):
        chain_early(0, step)

    @pl.loop(half, planes)
    def _(block):
        column_sums(block)

    table_finish(1)
    table_wait(1)

    build(1)

    def follow(unit):
        chain_begin(1, unit)
        chain_early(0, unit + row_blocks)
        chain_late(0, unit)
        chain_early(1, unit - 3 * row_blocks)
        chain_late(1, unit - 4 * row_blocks)

    @pl.loop(0, row_blocks)
    def _(step):
        begun = own[1, step].astype(jnp.float32)
        total = bands(lw_count, band_count, 0, sub_rows(step), kept[step], begun)
        own[1, step] = total.astype(own.dtype)
        follow(step)

    @pl.loop(1, planes)
    def _(block):
        gather_fields(block)

        @pl.loop(0, row_blocks)
        def _(step):
            unit = block * row_blocks + step
            rows = sub_rows(step)
            coarse = interpolate(block, rows)
            zero = jnp.zeros((width, BLOCK), jnp.float32)
            own[1, unit] = bands(0, band_count, block, rows, coarse, zero).astype(own.dtype)
            follow(unit)

    def finish_heat(block):
        for step in range(row_blocks):
            unit = block * row_blocks + step
            chain_ready(1, unit)
            heat[pl.ds(step * BLOCK, BLOCK), :] = jnp.transpose(chain_total(1, unit)).astype(jnp.bfloat16)
        moved = dot(btab[block], heat[...]).astype(jnp.bfloat16)
        tend_out[block] = moved.reshape(lon_count, segment, width)
        return_block(3, tend_out, block)

    @pl.loop(0, planes + 2)
    def _(turn):
        @pl.when(turn > 1)
        def _():
            finish_heat(turn - 2)

        @pl.when(turn < planes)
        def _():
            block = turn

            @pl.loop(0, row_blocks)
            def _(step):
                unit = block * row_blocks + step
                chain_ready(0, unit)
                rows = sub_rows(step)
                coarse = chain_total(0, unit)
                scale = scale_in[block, :, rows]
                lifted = jnp.concatenate(
                    [(scale[b : b + 1, :] * coarse).astype(jnp.bfloat16) for b in range(band_count)], axis=0
                )
                adj[:, rows] = dot(wide[...], lifted).astype(jnp.bfloat16)
                early, late = unit + units - 3 * row_blocks, unit + units - 4 * row_blocks

                @pl.when(block < 2)
                def _():
                    chain_early(1, early)

                @pl.when(block < planes - 1)
                def _():
                    chain_late(1, late)

                first = units - row_blocks + 2 * step

                @pl.when((block == 2) & (step < row_blocks // 2))
                def _():
                    chain_early(1, first)
                    chain_early(1, first + 1)

                @pl.when((block == planes - 1) & (step < row_blocks // 2))
                def _():
                    chain_late(1, first)
                    chain_late(1, first + 1)

            moved = lax.dot_general(ctab[block], adj[...], (((1,), (1,)), ((), ())), preferred_element_type=jnp.float32)
            grad_out[block] = moved.astype(jnp.bfloat16).reshape(lon_count, segment, flat_width)
            return_block(2, grad_out, block)

    for group in range(4):
        table_sent(group)

    if planes > 1:
        for kind in range(5):
            meta_whole(kind).wait_send()

    chain_sent(0)
    chain_sent(1)
    wait_sent(0, cot_out)
    wait_sent(1, fields_out)

    for block in range(early):
        wait_return(block)

    for kind, source in ((2, grad_out), (3, tend_out)):
        piece = source.at[:, 0]
        pltpu.make_async_copy(piece, piece, keep_sem.at[kind - 2]).wait()

    def put(step):
        rows = pl.ds(pl.multiple_of(step * FINAL, FINAL), FINAL)
        return pltpu.make_async_copy(staged.at[rows], restored.at[rows], put_sem)

    @pl.loop(0, col_count // FINAL)
    def _(step):
        rows = pl.ds(pl.multiple_of(step * FINAL, FINAL), FINAL)
        table = pick(perm_ref[:, pl.ds(0, early * part)] == row_iota(FINAL, early * part, step * FINAL))
        values = early_in[...].reshape(early * part, width + flat_width)
        staged[rows, :] = dot(table, values).astype(jnp.bfloat16)
        put(step).start()

    for block in range(early, planes):
        wait_return(block)
    pltpu.make_async_copy(staged, restored, put_sem).wait()

    wait_sent(2, grad_out)
    wait_sent(3, tend_out)


def restore_kernel(perm_ref, result_ref, restored_ref, tend_done, grad_done):
    rows, width = tend_done.shape
    late = result_ref.shape[0]
    slots = perm_ref[:, perm_ref.shape[1] - late :]
    table = pick(slots == row_iota(rows, late, pl.program_id(0) * rows))
    moved = (restored_ref[...].astype(jnp.float32) + dot(table, result_ref[...])).astype(jnp.bfloat16)
    tend_done[...] = moved[:, :width]
    for v in range(grad_done.shape[0]):
        grad_done[v] = moved[:, (v + 1) * width : (v + 2) * width]


def local(
    increments,
    cotangent,
    owner_perm,
    coarse_index,
    coarse_weight,
    back_index,
    back_weight,
    lw_scale,
    sw_scale,
    sunlit,
    lw_table,
    sw_table,
    *,
    planes,
    lon_count,
):
    col_count, var_count, width = increments.shape
    row_count = coarse_weight.shape[0]
    segment = col_count // (planes * lon_count)
    part = lon_count * segment
    flat_width = var_count * width
    thin, thick = (planes, lon_count, segment, width), (planes, lon_count, segment, flat_width)
    bands = lw_table.shape[0] + sw_table.shape[0]
    scale_rows = -(-(bands + 1) // 8) * 8
    wire = (2, planes * (row_count // BLOCK), width, BLOCK)
    half, full, whole = jnp.bfloat16, jnp.float32, jnp.int32
    vmem, hbm = pl.BlockSpec(memory_space=pltpu.VMEM), pl.BlockSpec(memory_space=pl.ANY)
    early = planes // 2
    stack_width = (var_count + 1) * width
    scratch = [
        ((early, lon_count, segment, stack_width), half),
        ((col_count, stack_width), half),
        ((col_count, (var_count + 1) * width), half),
        (thin, half),
        (thin, half),
        (thick, half),
        (thick, half),
        (thick, half),
        (thin, half),
        ((lon_count, bands) + lw_table.shape[1:], half),
        ((flat_width, bands * width), half),
        ((bands * width, flat_width), half),
        ((planes, part, row_count), half),
        ((planes, part, row_count), half),
        ((flat_width, part), half),
        ((row_count // BLOCK, flat_width, BLOCK), half),
        ((flat_width, row_count), half),
        ((row_count, width), half),
        (wire, half),
        (wire, half),
        (wire, half),
        (wire, half),
        (wire, full if planes * row_count <= WIDE_SUMS else half),
        ((planes, scale_rows, row_count), full),
        ((planes, 2, row_count), whole),
        ((planes, 1, row_count), full),
        ((planes, 2, part), whole),
        ((planes, 1, part), full),
    ]
    units = planes * (row_count // BLOCK)
    sems = (
        (4,),
        (4, planes),
        (2, 2),
        (2, 2, units),
        (5,),
        (5,),
        (4,),
        (4, lon_count),
        (2,),
        (3 + var_count,),
    )
    args = (
        owner_perm,
        jnp.transpose(increments, (1, 0, 2)),
        cotangent,
        back_index,
        back_weight[None, :],
        lw_scale,
        sw_scale,
        sunlit[None, :],
        lw_table,
        sw_table,
        coarse_index,
        coarse_weight[None, :],
    )
    result, restored = pl.pallas_call(
        radiate_kernel,
        out_shape=[
            jax.ShapeDtypeStruct((planes - early, lon_count, segment, stack_width), half),
            jax.ShapeDtypeStruct((col_count, stack_width), half),
        ],
        in_specs=[hbm if i in LOADED else vmem for i in range(len(args))],
        out_specs=[hbm, hbm],
        scratch_shapes=[pltpu.VMEM(shape, kind) for shape, kind in scratch]
        + [pltpu.SemaphoreType.DMA(shape) for shape in sems]
        + [pltpu.SemaphoreType.DMA],
        compiler_params=pltpu.CompilerParams(
            vmem_limit_bytes=62 * 1024 * 1024, has_side_effects=True, collective_id=0
        ),
        cost_estimate=pl.CostEstimate(
            flops=12 * planes * row_count * bands * flat_width * width, bytes_accessed=4 << 20, transcendentals=0
        ),
    )(*args)
    rows = 2 * FINAL
    steps = col_count // rows
    late = (planes - early) * part
    tendency, gradient = pl.pallas_call(
        restore_kernel,
        grid=(steps,),
        out_shape=[
            jax.ShapeDtypeStruct((col_count, width), half),
            jax.ShapeDtypeStruct((var_count, col_count, width), half),
        ],
        in_specs=[
            pl.BlockSpec((1, col_count), lambda i: (0, 0)),
            pl.BlockSpec((late, stack_width), lambda i: (0, 0)),
            pl.BlockSpec((rows, stack_width), lambda i: (i, 0)),
        ],
        out_specs=[
            pl.BlockSpec((rows, width), lambda i: (i, 0)),
            pl.BlockSpec((var_count, rows, width), lambda i: (0, i, 0)),
        ],
        compiler_params=pltpu.CompilerParams(vmem_limit_bytes=62 * 1024 * 1024),
        cost_estimate=pl.CostEstimate(
            flops=2 * col_count * late * stack_width, bytes_accessed=4 << 20, transcendentals=0
        ),
    )(owner_perm, result.reshape(late, stack_width), restored)
    return (tendency, jnp.transpose(gradient, (1, 0, 2)))


def solution(mesh):
    in_specs = (
        P(("lat", "lon"), None, None),
        P(("lat", "lon"), None),
        P(("lat", "lon"), None),
        P(None, ("lat", "lon")),
        P(("lat", "lon")),
        P(None, ("lat", "lon")),
        P(("lat", "lon")),
        P(None, ("lat", "lon")),
        P(None, ("lat", "lon")),
        P(("lat", "lon")),
        P(None, None, "lon", None),
        P(None, None, "lon", None),
    )
    out_specs = (P(("lat", "lon"), None), P(("lat", "lon"), None, None))

    def body(*args):
        return local(*args, planes=mesh.shape["lat"], lon_count=mesh.shape["lon"])

    return jax.shard_map(body, mesh=mesh, in_specs=in_specs, out_specs=out_specs, check_vma=False)
```

```python
import jax
import jax.numpy as jnp
from jax import lax
from jax.experimental import pallas as pl
from jax.experimental.pallas import tpu as pltpu
from jax.sharding import PartitionSpec as P

BLOCK = 256
FINAL = 512
BUNCH = 3
WIDE_SUMS = 4096
LOADED = (1, 2, 8, 9)


def lane_iota(rows, width):
    return lax.broadcasted_iota(jnp.int32, (rows, width), 1)


def row_iota(rows, width, start):
    return lax.broadcasted_iota(jnp.int32, (rows, width), 0) + start


def pick(hit):
    return jnp.where(hit, 1.0, 0.0).astype(jnp.bfloat16)


def blend(hit_first, hit_second, share):
    first = jnp.where(hit_first, share, 0.0)
    second = jnp.where(hit_second, 1.0 - share, 0.0)
    return (first + second).astype(jnp.bfloat16)


def dot(left, right):
    return lax.dot_general(left, right, (((1,), (0,)), ((), ())), preferred_element_type=jnp.float32)


def column_of(values):
    return jnp.transpose(jnp.broadcast_to(values, (8, values.shape[1])))[:, 0:1]


def radiate_kernel(
    perm_ref,
    inc_ref,
    cot_ref,
    back_ref,
    back_w,
    lw_scale,
    sw_scale,
    sun_ref,
    lw_ref,
    sw_ref,
    coarse_ref,
    coarse_w,
    result_in,
    restored,
    early_in,
    staged,
    stacked,
    cot_out,
    cot_in,
    fields_out,
    fields_in,
    grad_out,
    tend_out,
    tabs,
    wide,
    turned,
    ctab,
    btab,
    fields_t,
    kept,
    adj,
    heat,
    up_out,
    up_in,
    down_out,
    down_in,
    own,
    scale_in,
    coarse_in,
    share_in,
    back_in,
    back_share,
    send_sem,
    recv_sem,
    chain_send,
    chain_recv,
    meta_send,
    meta_recv,
    tab_send,
    tab_recv,
    keep_sem,
    load_sem,
    put_sem,
):
    var_count, col_count, width = inc_ref.shape
    planes, lon_count, segment = cot_out.shape[0], cot_out.shape[1], cot_out.shape[2]
    part = lon_count * segment
    row_count = lw_scale.shape[1]
    lw_count = lw_ref.shape[0]
    band_count = lw_count + sw_ref.shape[0]
    flat_width = var_count * width
    row_blocks = row_count // BLOCK
    units = planes * row_blocks
    half = planes // 2
    early = early_in.shape[0]
    lanes = (pl.ds(width, flat_width), pl.ds(0, width))
    lat, lon = lax.axis_index("lat"), lax.axis_index("lon")
    parity = lax.rem(lon, 2)
    partner = lon + 1 - 2 * parity
    lw_half, sw_half = lw_count // 2, lw_count + (band_count - lw_count) // 2
    edges = (0, lw_half, lw_count, sw_half, band_count)
    groups = tuple(pl.ds(edges[i], edges[i + 1] - edges[i]) for i in range(4))

    def remote(source, landing, send, recv, target_lat, target_lon):
        return pltpu.make_async_remote_copy(
            src_ref=source,
            dst_ref=landing,
            send_sem=send,
            recv_sem=recv,
            device_id=(target_lat, target_lon),
            device_id_type=pl.DeviceIdType.MESH,
        )

    def table_copy(group, slot, target):
        piece = tabs.at[slot, groups[group]]
        return remote(piece, piece, tab_send.at[group], tab_recv.at[group, slot], lat, target)

    quad = lon_count == 8
    if quad:
        across = lon + 2 - 4 * lax.rem(lax.div(lon, 2), 2)
        along = lon + 4 - 8 * lax.div(lon, 4)
        near, far = (across, along), across + along - lon
    else:
        near, far = tuple(lax.rem(lon + 2 * j, lon_count) for j in range(1, lon_count // 2)), None

    def relay(group):
        return table_copy(group, near[group % 2], near[1 - group % 2])

    def table_start(side):
        for group in (2 * side, 2 * side + 1):
            for target in near + (partner,):
                table_copy(group, lon, target).start()

    def table_relay(side):
        for group in (2 * side, 2 * side + 1):
            for source in near:
                table_copy(group, source, source).wait_recv()
            if quad:
                relay(group).start()
            for source in near:
                table_copy(group, source, partner).start()

    def table_finish(side):
        if quad:
            for group in (2 * side, 2 * side + 1):
                table_copy(group, far, far).wait_recv()
                table_copy(group, far, partner).start()

    def table_wait(side):
        for group in (2 * side, 2 * side + 1):
            for j in range(lon_count // 2):
                source = lax.rem(partner + 2 * j, lon_count)
                table_copy(group, source, source).wait_recv()

    def table_sent(group):
        pieces = tabs.at[pl.ds(0, lon_count - 1), groups[group]]
        remote(pieces, pieces, tab_send.at[group], tab_recv.at[group, 0], lat, partner).wait_send()

    def copy(kind, source, landing, block, target):
        return remote(source, landing, send_sem.at[kind], recv_sem.at[kind, block], lat, target)

    def start_block(kind, source, landing, block, spot=None):
        spot = block if spot is None else spot
        landing = landing.at[spot, lon]
        if kind < 2:
            landing[...] = source[block, lon]
        else:
            pltpu.make_async_copy(source.at[block, lon], landing, keep_sem.at[kind - 2]).start()

        @pl.loop(1, lon_count)
        def _(k):
            target = lax.rem(lon + k, lon_count)
            copy(kind, source.at[block, target], landing, block, target).start()

    def return_block(kind, source, block):
        @pl.when(block < early)
        def _():
            start_block(kind, source, early_in.at[:, :, :, lanes[kind - 2]], block)

        @pl.when(block >= early)
        def _():
            start_block(kind, source, result_in.at[:, :, :, lanes[kind - 2]], block, block - early)

    def wait_return(block):
        for kind, landing in ((2, grad_out), (3, tend_out)):
            wait_block(kind, landing, block)

    def wait_block(kind, landing, block):
        pieces = landing.at[block, pl.ds(0, lon_count - 1)]
        copy(kind, pieces, pieces, block, partner).wait_recv()

    def wait_sent(kind, source):
        pieces = source.at[:, pl.ds(0, lon_count - 1)]
        copy(kind, pieces, pieces, 0, partner).wait_send()

    def meta_copy(kind, target, slot):
        span = pl.ds(pl.multiple_of(target * part, part), part)
        source, landing = (
            (back_ref.at[:, span], back_in.at[slot]),
            (back_w.at[:, span], back_share.at[slot]),
            (coarse_ref, coarse_in.at[slot]),
            (coarse_w, share_in.at[slot]),
            (scale_in.at[slot], scale_in.at[slot]),
        )[kind]
        return remote(source, landing, meta_send.at[kind], meta_recv.at[kind], target, lon)

    def meta_whole(kind):
        pieces = (back_in, back_share, coarse_in, share_in, scale_in)[kind].at[pl.ds(0, planes - 1)]
        return remote(pieces, pieces, meta_send.at[kind], meta_recv.at[kind], lat, partner)

    def wait_meta(kinds):
        if planes > 1:
            for kind in kinds:
                meta_whole(kind).wait_recv()

    def chain_copy(kind, upward, unit):
        out, landing, way = (up_out, up_in, 0) if upward else (down_out, down_in, 1)
        target = lat + 1 if upward else lat - 1
        piece, spot = out.at[kind, unit], landing.at[kind, unit]
        return remote(piece, spot, chain_send.at[kind, way], chain_recv.at[kind, way, unit], target, lon)

    def chain_begin(kind, unit):
        if planes == 1:
            return

        @pl.when(lat == 0)
        def _():
            up_out[kind, unit] = own[kind, unit].astype(jnp.bfloat16)
            chain_copy(kind, True, unit).start()

        @pl.when(lat == planes - 1)
        def _():
            down_out[kind, unit] = own[kind, unit].astype(jnp.bfloat16)
            chain_copy(kind, False, unit).start()

    def chain_hop(kind, hop, unit):
        @pl.when((lat == hop) & (unit >= 0) & (unit < units))
        def _():
            chain_copy(kind, True, unit).wait_recv()
            up_out[kind, unit] = (own[kind, unit].astype(jnp.float32) + up_in[kind, unit].astype(jnp.float32)).astype(jnp.bfloat16)
            chain_copy(kind, True, unit).start()

        @pl.when((lat == planes - 1 - hop) & (unit >= 0) & (unit < units))
        def _():
            chain_copy(kind, False, unit).wait_recv()
            down_out[kind, unit] = (own[kind, unit].astype(jnp.float32) + down_in[kind, unit].astype(jnp.float32)).astype(jnp.bfloat16)
            chain_copy(kind, False, unit).start()

    def chain_late(kind, unit):
        for hop in range(2, planes - 1):
            chain_hop(kind, hop, unit)

    def chain_early(kind, unit):
        if planes > 2:
            chain_hop(kind, 1, unit)

    def chain_ready(kind, unit):
        if planes == 1:
            return

        @pl.when(lat == 0)
        def _():
            chain_copy(kind, False, unit).wait_recv()

        @pl.when(lat == planes - 1)
        def _():
            chain_copy(kind, True, unit).wait_recv()

    def chain_total(kind, unit):
        ends = up_in[kind, unit].astype(jnp.float32) + down_in[kind, unit].astype(jnp.float32)
        return own[kind, unit].astype(jnp.float32) + ends

    def chain_sent(kind):
        @pl.when(lat < planes - 1)
        def _():
            pieces = up_out.at[kind]
            remote(pieces, pieces, chain_send.at[kind, 0], chain_recv.at[kind, 0, 0], lat, partner).wait_send()

        @pl.when(lat > 0)
        def _():
            pieces = down_out.at[kind]
            remote(pieces, pieces, chain_send.at[kind, 1], chain_recv.at[kind, 1, 0], lat, partner).wait_send()

    def sub_rows(step):
        return pl.ds(pl.multiple_of(step * BLOCK, BLOCK), BLOCK)

    barrier = pltpu.get_barrier_semaphore()
    for k in range(1, lon_count):
        pl.semaphore_signal(
            barrier, inc=1, device_id=(lat, lax.rem(lon + k, lon_count)), device_id_type=pl.DeviceIdType.MESH
        )
    for k in range(1, planes):
        pl.semaphore_signal(
            barrier, inc=1, device_id=(lax.rem(lat + k, planes), lon), device_id_type=pl.DeviceIdType.MESH
        )
    loads = [
        pltpu.make_async_copy(lw_ref, tabs.at[lon, pl.ds(0, lw_count)], load_sem.at[0]),
        pltpu.make_async_copy(sw_ref, tabs.at[lon, pl.ds(lw_count, band_count - lw_count)], load_sem.at[1]),
        pltpu.make_async_copy(cot_ref, stacked.at[:, pl.ds(0, width)], load_sem.at[2]),
    ] + [
        pltpu.make_async_copy(inc_ref.at[v], stacked.at[:, pl.ds((v + 1) * width, width)], load_sem.at[3 + v])
        for v in range(var_count)
    ]
    for load in loads:
        load.start()
    scale_in[lat, pl.ds(0, lw_count)] = lw_scale[...]
    scale_in[lat, pl.ds(lw_count, band_count - lw_count)] = sw_scale[...] * sun_ref[...].astype(jnp.float32)
    scale_in[lat, pl.ds(band_count, scale_in.shape[1] - band_count)] = jnp.zeros(
        (scale_in.shape[1] - band_count, row_count), jnp.float32
    )
    span = pl.ds(pl.multiple_of(lat * part, part), part)
    back_in[lat] = back_ref[:, span]
    back_share[lat] = back_w[:, span]
    coarse_in[lat] = coarse_ref[...]
    share_in[lat] = coarse_w[...]

    @pl.when(lat == 0)
    def _():
        up_in[...] = jnp.zeros_like(up_in)

    @pl.when(lat == planes - 1)
    def _():
        down_in[...] = jnp.zeros_like(down_in)

    loads[0].wait()
    loads[1].wait()

    pl.semaphore_wait(barrier, lon_count + planes - 2)
    table_start(0)
    for kinds in ((0, 1), (2, 3, 4)):
        for k in range(1, planes):
            for kind in kinds:
                meta_copy(kind, lax.rem(lat + k, planes), lat).start()

    for load in loads[2:]:
        load.wait()

    @pl.loop(0, planes)
    def _(block):
        rows = pl.ds(pl.multiple_of(block * part, part), part)
        table = pick(column_of(perm_ref[:, rows]) == lane_iota(part, col_count))
        moved = dot(table, stacked[...]).astype(jnp.bfloat16)
        cot_out[block] = moved[:, :width].reshape(lon_count, segment, width)
        fields_out[block] = moved[:, width:].reshape(lon_count, segment, flat_width)

        @pl.when(block < half)
        def _():
            start_block(0, cot_out, cot_in, block)

    table_relay(0)
    start_block(1, fields_out, fields_in, 0)
    table_start(1)

    @pl.loop(half, planes)
    def _(block):
        start_block(0, cot_out, cot_in, block)

    wait_meta((0, 1))

    @pl.loop(0, planes)
    def _(block):
        spot = lane_iota(part, row_count)
        first, second = column_of(back_in[block, 0:1, :]), column_of(back_in[block, 1:2, :])
        btab[block] = blend(first == spot, second == spot, column_of(back_share[block]))

    def column_sums(block):
        wait_block(0, cot_in, block)
        partial = dot(jnp.transpose(cot_in[block].reshape(part, width)), btab[block])
        for step in range(row_blocks):
            own[0, block * row_blocks + step] = partial[:, step * BLOCK : (step + 1) * BLOCK].astype(own.dtype)
            chain_begin(0, block * row_blocks + step)

    @pl.loop(0, half)
    def _(block):
        column_sums(block)

    def build(group):
        depth = lw_ref.shape[2]
        for b in range(lw_count) if group == 0 else range(lw_count, band_count):
            for v in range(var_count):
                piece = tabs[:, b, v].reshape(lon_count * depth, width)
                wide[pl.ds(v * lon_count * depth, lon_count * depth), pl.ds(b * width, width)] = piece
                turned[pl.ds(b * width, width), pl.ds(v * lon_count * depth, lon_count * depth)] = jnp.transpose(piece)

    def bands(first, last, block, rows, coarse, total):
        scale = scale_in[block, :, rows]
        for start in range(first, last, BUNCH):
            stop = min(start + BUNCH, last)
            bunch = dot(turned[start * width : stop * width, :], coarse)
            for b in range(start, stop):
                total = total + scale[b : b + 1, :] * bunch[(b - start) * width : (b - start + 1) * width, :]
        return total

    def gather_fields(block):
        wait_block(1, fields_in, block)
        fields_t[...] = jnp.transpose(fields_in[block].reshape(part, flat_width))

    def interpolate(block, rows):
        spot = row_iota(part, BLOCK, lat * part)
        index = coarse_in[block, :, rows]
        table = blend(index[0:1, :] == spot, index[1:2, :] == spot, share_in[block, :, rows])
        ctab[block, :, rows] = table
        return dot(fields_t[...], table).astype(jnp.bfloat16)

    table_finish(0)
    table_wait(0)

    build(0)
    wait_meta((2, 3, 4))

    gather_fields(0)

    @pl.loop(0, row_blocks)
    def _(step):
        rows = sub_rows(step)
        coarse = interpolate(0, rows)
        kept[step] = coarse
        own[1, step] = bands(0, lw_count, 0, rows, coarse, jnp.zeros((width, BLOCK), jnp.float32)).astype(own.dtype)

    table_relay(1)

    @pl.loop(1, planes)
    def _(block):
        start_block(1, fields_out, fields_in, block)

    @pl.loop(0, row_blocks)
    def _(step):
        chain_early(0, step)

    @pl.loop(half, planes)
    def _(block):
        column_sums(block)

    table_finish(1)
    table_wait(1)

    build(1)

    def follow(unit):
        chain_begin(1, unit)
        chain_early(0, unit + row_blocks)
        chain_late(0, unit)
        chain_early(1, unit - 3 * row_blocks)
        chain_late(1, unit - 4 * row_blocks)

    @pl.loop(0, row_blocks)
    def _(step):
        begun = own[1, step].astype(jnp.float32)
        total = bands(lw_count, band_count, 0, sub_rows(step), kept[step], begun)
        own[1, step] = total.astype(own.dtype)
        follow(step)

    @pl.loop(1, planes)
    def _(block):
        gather_fields(block)

        @pl.loop(0, row_blocks)
        def _(step):
            unit = block * row_blocks + step
            rows = sub_rows(step)
            coarse = interpolate(block, rows)
            zero = jnp.zeros((width, BLOCK), jnp.float32)
            own[1, unit] = bands(0, band_count, block, rows, coarse, zero).astype(own.dtype)
            follow(unit)

    def finish_heat(block):
        for step in range(row_blocks):
            unit = block * row_blocks + step
            chain_ready(1, unit)
            heat[pl.ds(step * BLOCK, BLOCK), :] = jnp.transpose(chain_total(1, unit)).astype(jnp.bfloat16)
        moved = dot(btab[block], heat[...]).astype(jnp.bfloat16)
        tend_out[block] = moved.reshape(lon_count, segment, width)
        return_block(3, tend_out, block)

    delay = jnp.where((lat == 0) | (lat == planes - 1), 2, 1)

    @pl.loop(0, planes + 2)
    def _(turn):
        @pl.when((turn >= delay) & (turn < planes + delay))
        def _():
            finish_heat(turn - delay)

        @pl.when(turn < planes)
        def _():
            block = turn

            @pl.loop(0, row_blocks)
            def _(step):
                unit = block * row_blocks + step
                chain_ready(0, unit)
                rows = sub_rows(step)
                coarse = chain_total(0, unit)
                scale = scale_in[block, :, rows]
                lifted = jnp.concatenate(
                    [(scale[b : b + 1, :] * coarse).astype(jnp.bfloat16) for b in range(band_count)], axis=0
                )
                adj[:, rows] = dot(wide[...], lifted).astype(jnp.bfloat16)
                early, late = unit + units - 3 * row_blocks, unit + units - 4 * row_blocks

                @pl.when(block < 2)
                def _():
                    chain_early(1, early)

                @pl.when(block < 3)
                def _():
                    chain_late(1, late)

                first = units - row_blocks + 2 * step

                @pl.when((block == 2) & (step < row_blocks // 2))
                def _():
                    chain_early(1, first)
                    chain_early(1, first + 1)

                @pl.when((block == 3) & (step < row_blocks // 2))
                def _():
                    chain_late(1, first)
                    chain_late(1, first + 1)

            moved = lax.dot_general(ctab[block], adj[...], (((1,), (1,)), ((), ())), preferred_element_type=jnp.float32)
            grad_out[block] = moved.astype(jnp.bfloat16).reshape(lon_count, segment, flat_width)
            return_block(2, grad_out, block)

    for group in range(4):
        table_sent(group)

    if planes > 1:
        for kind in range(5):
            meta_whole(kind).wait_send()

    chain_sent(0)
    chain_sent(1)
    wait_sent(0, cot_out)
    wait_sent(1, fields_out)

    for block in range(early):
        wait_return(block)

    for kind, source in ((2, grad_out), (3, tend_out)):
        piece = source.at[:, 0]
        pltpu.make_async_copy(piece, piece, keep_sem.at[kind - 2]).wait()

    def put(step):
        rows = pl.ds(pl.multiple_of(step * FINAL, FINAL), FINAL)
        return pltpu.make_async_copy(staged.at[rows], restored.at[rows], put_sem)

    @pl.loop(0, col_count // FINAL)
    def _(step):
        rows = pl.ds(pl.multiple_of(step * FINAL, FINAL), FINAL)
        table = pick(perm_ref[:, pl.ds(0, early * part)] == row_iota(FINAL, early * part, step * FINAL))
        values = early_in[...].reshape(early * part, width + flat_width)
        staged[rows, :] = dot(table, values).astype(jnp.bfloat16)
        put(step).start()

    for block in range(early, planes):
        wait_return(block)
    pltpu.make_async_copy(staged, restored, put_sem).wait()

    wait_sent(2, grad_out)
    wait_sent(3, tend_out)


def restore_kernel(perm_ref, result_ref, restored_ref, tend_done, grad_done):
    rows, width = tend_done.shape
    late = result_ref.shape[0]
    slots = perm_ref[:, perm_ref.shape[1] - late :]
    table = pick(slots == row_iota(rows, late, pl.program_id(0) * rows))
    moved = (restored_ref[...].astype(jnp.float32) + dot(table, result_ref[...])).astype(jnp.bfloat16)
    tend_done[...] = moved[:, :width]
    for v in range(grad_done.shape[0]):
        grad_done[v] = moved[:, (v + 1) * width : (v + 2) * width]


def local(
    increments,
    cotangent,
    owner_perm,
    coarse_index,
    coarse_weight,
    back_index,
    back_weight,
    lw_scale,
    sw_scale,
    sunlit,
    lw_table,
    sw_table,
    *,
    planes,
    lon_count,
):
    col_count, var_count, width = increments.shape
    row_count = coarse_weight.shape[0]
    segment = col_count // (planes * lon_count)
    part = lon_count * segment
    flat_width = var_count * width
    thin, thick = (planes, lon_count, segment, width), (planes, lon_count, segment, flat_width)
    bands = lw_table.shape[0] + sw_table.shape[0]
    scale_rows = -(-(bands + 1) // 8) * 8
    wire = (2, planes * (row_count // BLOCK), width, BLOCK)
    half, full, whole = jnp.bfloat16, jnp.float32, jnp.int32
    vmem, hbm = pl.BlockSpec(memory_space=pltpu.VMEM), pl.BlockSpec(memory_space=pl.ANY)
    early = planes // 2
    stack_width = (var_count + 1) * width
    scratch = [
        ((early, lon_count, segment, stack_width), half),
        ((col_count, stack_width), half),
        ((col_count, (var_count + 1) * width), half),
        (thin, half),
        (thin, half),
        (thick, half),
        (thick, half),
        (thick, half),
        (thin, half),
        ((lon_count, bands) + lw_table.shape[1:], half),
        ((flat_width, bands * width), half),
        ((bands * width, flat_width), half),
        ((planes, part, row_count), half),
        ((planes, part, row_count), half),
        ((flat_width, part), half),
        ((row_count // BLOCK, flat_width, BLOCK), half),
        ((flat_width, row_count), half),
        ((row_count, width), half),
        (wire, half),
        (wire, half),
        (wire, half),
        (wire, half),
        (wire, full if planes * row_count <= WIDE_SUMS else half),
        ((planes, scale_rows, row_count), full),
        ((planes, 2, row_count), whole),
        ((planes, 1, row_count), full),
        ((planes, 2, part), whole),
        ((planes, 1, part), full),
    ]
    units = planes * (row_count // BLOCK)
    sems = (
        (4,),
        (4, planes),
        (2, 2),
        (2, 2, units),
        (5,),
        (5,),
        (4,),
        (4, lon_count),
        (2,),
        (3 + var_count,),
    )
    args = (
        owner_perm,
        jnp.transpose(increments, (1, 0, 2)),
        cotangent,
        back_index,
        back_weight[None, :],
        lw_scale,
        sw_scale,
        sunlit[None, :],
        lw_table,
        sw_table,
        coarse_index,
        coarse_weight[None, :],
    )
    result, restored = pl.pallas_call(
        radiate_kernel,
        out_shape=[
            jax.ShapeDtypeStruct((planes - early, lon_count, segment, stack_width), half),
            jax.ShapeDtypeStruct((col_count, stack_width), half),
        ],
        in_specs=[hbm if i in LOADED else vmem for i in range(len(args))],
        out_specs=[hbm, hbm],
        scratch_shapes=[pltpu.VMEM(shape, kind) for shape, kind in scratch]
        + [pltpu.SemaphoreType.DMA(shape) for shape in sems]
        + [pltpu.SemaphoreType.DMA],
        compiler_params=pltpu.CompilerParams(
            vmem_limit_bytes=62 * 1024 * 1024, has_side_effects=True, collective_id=0
        ),
        cost_estimate=pl.CostEstimate(
            flops=12 * planes * row_count * bands * flat_width * width, bytes_accessed=4 << 20, transcendentals=0
        ),
    )(*args)
    rows = 2 * FINAL
    steps = col_count // rows
    late = (planes - early) * part
    tendency, gradient = pl.pallas_call(
        restore_kernel,
        grid=(steps,),
        out_shape=[
            jax.ShapeDtypeStruct((col_count, width), half),
            jax.ShapeDtypeStruct((var_count, col_count, width), half),
        ],
        in_specs=[
            pl.BlockSpec((1, col_count), lambda i: (0, 0)),
            pl.BlockSpec((late, stack_width), lambda i: (0, 0)),
            pl.BlockSpec((rows, stack_width), lambda i: (i, 0)),
        ],
        out_specs=[
            pl.BlockSpec((rows, width), lambda i: (i, 0)),
            pl.BlockSpec((var_count, rows, width), lambda i: (0, i, 0)),
        ],
        compiler_params=pltpu.CompilerParams(vmem_limit_bytes=62 * 1024 * 1024),
        cost_estimate=pl.CostEstimate(
            flops=2 * col_count * late * stack_width, bytes_accessed=4 << 20, transcendentals=0
        ),
    )(owner_perm, result.reshape(late, stack_width), restored)
    return (tendency, jnp.transpose(gradient, (1, 0, 2)))


def solution(mesh):
    in_specs = (
        P(("lat", "lon"), None, None),
        P(("lat", "lon"), None),
        P(("lat", "lon"), None),
        P(None, ("lat", "lon")),
        P(("lat", "lon")),
        P(None, ("lat", "lon")),
        P(("lat", "lon")),
        P(None, ("lat", "lon")),
        P(None, ("lat", "lon")),
        P(("lat", "lon")),
        P(None, None, "lon", None),
        P(None, None, "lon", None),
    )
    out_specs = (P(("lat", "lon"), None), P(("lat", "lon"), None, None))

    def body(*args):
        return local(*args, planes=mesh.shape["lat"], lon_count=mesh.shape["lon"])

    return jax.shard_map(body, mesh=mesh, in_specs=in_specs, out_specs=out_specs, check_vma=False)
```
